32 devices in a mesh: gx: 8 (over z, core), gy: 4 (over y, x).
Axes of the slice: x: 2, y: 2, z: 4, core: 2. Of those that a mesh axis runs over, the one named last changes fastest.
Arguments:
- right_side: float32 [128, 128, 128], P('gx', 'gy'), may hold values from -6 to 6
- shift: float32 [128, 128, 128], P('gx', 'gy'), may hold values from 0.5 to 8
Outputs:
- solution_field: float32 [128, 128, 128], P('gx', 'gy')
- residual: float32 [128, 128, 128], P('gx', 'gy')
The draws below stay inside these ranges and needn't reach their ends.
All inputs are finite; a program needn't handle non-finite values.
Results may differ from the reference program's by a relative error of at most 0.0003.
Values sent between devices are 32-bit elements; how exact they have to be, the bound alone decides.
A program may use at most 128 MiB of HBM per device.

```python
import math
import jax
import jax.numpy as jnp
from jax import lax

CX = 16
CY = 32
CZ = 128
ITERS = 3
LEVELS = 3
SWEEPS = 2
BOTTOM = 4
NX = 128
NY = 128
N_GX = 8
N_GY = 4


def shard_levels(own_key, dims, cuts, least, top_value):
    def one(dim, blocks):
        steps = jax.random.uniform(jax.random.fold_in(jax.random.fold_in(own_key, 6), dim), (blocks,), jnp.float32, least / len(cuts), top_value / len(cuts))
        return jnp.repeat(jnp.exp(steps), dims[dim] // blocks).reshape((-1,) + (1,) * (len(dims) - dim - 1))

    factor_of = one(*cuts[0])
    for cut in cuts[1:]:
        factor_of = factor_of * one(*cut)
    return factor_of


def normal_values(rng, shape, scale, bound, split=(), held_as=jnp.bfloat16):
    values = scale * jax.random.normal(rng, shape, jnp.float32)
    if split:
        values = values * shard_levels(rng, shape, split, -0.22, 0.18)
    return jnp.clip(values, -bound, bound).astype(held_as)


def setup_inputs(seed: int = 0) -> dict:
    splits = jax.random.split(jax.random.key(seed), 3)
    return {
        "right_side": normal_values(splits[0], (NX, NY, CZ), 1.0, 6.0, ((0, 8), (1, 4)), jnp.float32),
        "shift": jnp.clip(jnp.exp(math.log(8.0) - 2.7725887 * jax.random.uniform(splits[1], (NX, NY, CZ), jnp.float32) ** shard_levels(splits[1], (NX, NY, CZ), ((0, 8), (1, 4)), -0.2, 0.2)), 0.5, 8.0),
    }


relaxation = 0.7
center_weight = 26.0


def neighbours(padded):
    total = padded[:, :, :-2] + padded[:, :, 1:-1] + padded[:, :, 2:]
    total = total[:, :-2] + total[:, 1:-1] + total[:, 2:]
    total = total[:-2] + total[1:-1] + total[2:]
    return total - padded[1:-1, 1:-1, 1:-1]


def coarsen(field):
    first, second, third = field.shape
    return field.reshape(first // 2, 2, second // 2, 2, third // 2, 2).mean(axis=(1, 3, 5))


def prolong(field):
    return jnp.repeat(jnp.repeat(jnp.repeat(field, 2, 0), 2, 1), 2, 2)


def level_diagonals(box_shift):
    result = []
    current = box_shift
    for level in range(LEVELS):
        result.append(center_weight + (4.0 ** level) * current)
        if level + 1 < LEVELS:
            current = coarsen(current)
    return result


def sweep(guess, source, diag):
    return guess + relaxation * (source - (diag * guess - neighbours(jnp.pad(guess, 1)))) / diag


def vcycle(rhs, diags, level):
    diag = diags[level]
    source = (4.0 ** level) * rhs
    count = BOTTOM if level == LEVELS - 1 else SWEEPS
    guess = relaxation * source / diag
    for turn in range(count - 1):
        guess = sweep(guess, source, diag)
    if level < LEVELS - 1:
        leftover = (source - (diag * guess - neighbours(jnp.pad(guess, 1)))) / (4.0 ** level)
        guess = guess + prolong(vcycle(coarsen(leftover), diags, level + 1))
        for turn in range(SWEEPS):
            guess = sweep(guess, source, diag)
    return guess


def precondition(residual, shift):
    widths = ((2, 2), (2, 2), (0, 0))
    res_pad = jnp.pad(residual, widths)
    shift_pad = jnp.pad(shift, widths)
    total = jnp.zeros_like(res_pad)
    extent = (CX + 4, CY + 4, CZ)

    def visit(total, index):
        start_x = ((index // N_GY) * CX).astype(jnp.int32)
        start_y = ((index % N_GY) * CY).astype(jnp.int32)
        start = (start_x, start_y, jnp.zeros((), jnp.int32))
        box = lax.dynamic_slice(res_pad, start, extent)
        box_shift = lax.dynamic_slice(shift_pad, start, extent)
        local = vcycle(box, level_diagonals(box_shift), 0)
        older = lax.dynamic_slice(total, start, extent)
        return lax.dynamic_update_slice(total, older + local, start), None

    total, unused = lax.scan(visit, total, jnp.arange(N_GX * N_GY, dtype=jnp.int32))
    return total[2:-2, 2:-2]


def operate(field, shift):
    return (center_weight + shift) * field - neighbours(jnp.pad(field, 1))


def reference(right_side, shift):
    solution_field = jnp.zeros_like(right_side)
    residual = right_side
    precond = precondition(residual, shift)
    direction = precond
    rz_now = jnp.sum(residual * precond)
    for step in range(ITERS):
        image = operate(direction, shift)
        alpha = rz_now / jnp.sum(direction * image)
        solution_field = solution_field + alpha * direction
        residual = residual - alpha * image
        if step + 1 < ITERS:
            precond = precondition(residual, shift)
            rz_next = jnp.sum(residual * precond)
            direction = precond + (rz_next / rz_now) * direction
            rz_now = rz_next
    return solution_field, residual
```

```python
import functools

import jax
import jax.numpy as jnp
from jax import lax
from jax.experimental import pallas as pl
from jax.experimental.pallas import tpu as pltpu
from jax.sharding import PartitionSpec as P

MESH = pl.DeviceIdType.MESH
ROUNDS = 3
SWEEPS = 2
BOTTOM = 4
CENTER = 26.0
RELAX = 0.7
KEEP = 1.0 - RELAX
THETA = 1.0

SIDES = [(-1, 0), (1, 0), (0, -1), (0, 1)]
CORNERS = [(-1, -1), (-1, 1), (1, -1), (1, 1)]


def loop(count, body):
    def step(i, carry):
        body(i)
        return carry

    lax.fori_loop(0, count, step, 0)


def kernel(
    gx, gy, X, Y, Z,
    rhs, shf, out_x, out_r,
    g0, dA, wc0, e1, eA, eB, vbox, vext, wext,
    wc1, dd1, g1, e1b, eAb, eBb, wc2, e1c, eAc, eBc,
    pack, in_x, in_y, in_c, rx, ry, rc, gram,
    is_sem, ir_sem, s_sem, r_sem, gs_sem, gr_sem,
):
    n = gx * gy
    R = Y + 8
    n0, n1, n2 = X + 4, (X + 4) // 2, (X + 4) // 4
    ix, iy = lax.axis_index("gx"), lax.axis_index("gy")
    me = ix * gy + iy

    def there(dx, dy):
        ok = None
        for d, i, c in ((dx, ix, gx), (dy, iy, gy)):
            if d:
                here = (i > 0) if d < 0 else (i < c - 1)
                ok = here if ok is None else jnp.logical_and(ok, here)
        return ok

    def clear(refs):
        for ref in refs:
            lead = ref.shape[:-2] if len(ref.shape) == 3 else ref.shape[:-3]

            def body(i, ref=ref, lead=lead):
                at = (i,) if len(lead) == 1 else (i // lead[1], lax.rem(i, lead[1]))
                ref[at] = jnp.zeros(ref.shape[len(lead):], jnp.float32)

            loop(lead[0] if len(lead) == 1 else lead[0] * lead[1], body)

    clear((in_x, in_y, in_c, rx, ry, rc))
    barrier = pltpu.get_barrier_semaphore()

    @pl.loop(1, n)
    def _(d):
        other = lax.rem(me + d, n)
        pl.semaphore_signal(
            barrier, inc=1, device_id=(other // gy, lax.rem(other, gy)), device_id_type=MESH
        )

    clear((eA, eB, e1, vbox, g0, dA, eAb, eBb, e1b, eAc, eBc, e1c))

    pack[0, :, 0:2, :] = rhs[:, 0:2, :]
    pack[0, :, 2:4, :] = shf[:, 0:2, :]
    pack[1, :, 0:2, :] = rhs[:, Y - 2:Y, :]
    pack[1, :, 2:4, :] = shf[:, Y - 2:Y, :]
    pack[:, :, 4:8, :] = jnp.zeros((2, X, 4, Z), jnp.float32)

    pl.semaphore_wait(barrier, n - 1)

    def remote(src, dst, ss, rs, dx, dy):
        return pltpu.make_async_remote_copy(
            src_ref=src, dst_ref=dst, send_sem=ss, recv_sem=rs,
            device_id=(ix + dx, iy + dy), device_id_type=MESH,
        )

    def flip(k):
        return k ^ 1

    def first_copies():
        result = []
        for k, (dx, dy) in enumerate(SIDES):
            if dx:
                at = 0 if dx < 0 else X - 2
                for a, ref in enumerate((rhs, shf)):
                    result.append((dx, dy, ref.at[pl.ds(at, 2)], in_x.at[k ^ 1, a],
                                   2 * k + a, 2 * (k ^ 1) + a))
            else:
                result.append((dx, dy, pack.at[k - 2], in_y.at[(k - 2) ^ 1],
                               2 + k, 2 + (k ^ 1)))
        for k, (dx, dy) in enumerate(CORNERS):
            at = 0 if dx < 0 else X - 2
            row = 0 if dy < 0 else 1
            result.append((dx, dy, pack.at[row, pl.ds(at, 2)], in_c.at[3 - k], 6 + k, 6 + 3 - k))
        return result

    def back_copies(r):
        result = []
        box = vbox.at[r]
        for k, (dx, dy) in enumerate(SIDES):
            if dx:
                src = box.at[pl.ds(1 if dx < 0 else X, 5)]
                result.append((dx, dy, src, rx.at[r, k ^ 1], k, k ^ 1))
            else:
                src = box.at[pl.ds(1, n0), pl.ds(0 if dy < 0 else Y, 8)]
                result.append((dx, dy, src, ry.at[r, (k - 2) ^ 1], k, k ^ 1))
        for k, (dx, dy) in enumerate(CORNERS):
            src = box.at[pl.ds(1 if dx < 0 else X, 5), pl.ds(0 if dy < 0 else Y, 8)]
            result.append((dx, dy, src, rc.at[r, 3 - k], 4 + k, 4 + 3 - k))
        return result

    def start(copies, ss, rs):
        for dx, dy, src, dst, a, b in copies:
            @pl.when(there(dx, dy))
            def _(dx=dx, dy=dy, src=src, dst=dst, a=a, b=b):
                remote(src, dst, ss.at[a], rs.at[b], dx, dy).start()

    def arrive(copies, ss, rs):
        for dx, dy, src, dst, a, b in copies:
            @pl.when(there(-dx, -dy))
            def _(dx=dx, dy=dy, src=src, dst=dst, a=a, b=b):
                remote(src, dst, ss.at[a], rs.at[b], -dx, -dy).wait_recv()

    def leave(copies, ss, rs):
        for dx, dy, src, dst, a, b in copies:
            @pl.when(there(dx, dy))
            def _(dx=dx, dy=dy, src=src, dst=dst, a=a, b=b):
                remote(src, dst, ss.at[a], rs.at[b], dx, dy).wait_send()

    firsts = first_copies()
    start(firsts, is_sem, ir_sem)

    row = lax.broadcasted_iota(jnp.int32, (1, R, Z), 1)
    lane = lax.broadcasted_iota(jnp.int32, (1, R, Z), 2)

    g0[2:X + 2, 3:Y + 3, :] = rhs[...]
    dA[2:X + 2, 3:Y + 3, :] = shf[...]

    arrive(firsts, is_sem, ir_sem)
    for ref, a in ((g0, 0), (dA, 1)):
        ref[0:2, 3:Y + 3, :] = in_x[0, a]
        ref[X + 2:X + 4, 3:Y + 3, :] = in_x[1, a]
        ref[2:X + 2, 1:3, :] = in_y[0, :, 2 * a:2 * a + 2, :]
        ref[2:X + 2, Y + 3:Y + 5, :] = in_y[1, :, 2 * a:2 * a + 2, :]
        for k, (dx, dy) in enumerate(CORNERS):
            s = 0 if dx < 0 else X + 2
            t = 1 if dy < 0 else Y + 3
            ref[s:s + 2, t:t + 2, :] = in_c[k, :, 2 * a:2 * a + 2, :]

    in_box = jnp.logical_and(row >= 1, row <= Y + 4)
    relax = jnp.where(in_box, RELAX, 0.0).astype(jnp.float32)
    at_y = iy * Y + row - 3
    in_grid = jnp.where(
        jnp.logical_and(at_y >= 0, at_y < gy * Y), 1.0, 0.0
    ).astype(jnp.float32)

    def pair_sum(t, k):
        first = lax.rem(jnp.maximum(row - 1, 0) // k, 2) == 0
        t = t + jnp.where(first, pltpu.roll(t, R - k, 1), pltpu.roll(t, k, 1))
        low = lax.rem(lane // k, 2) == 0
        return t + jnp.where(low, pltpu.roll(t, Z - k, 2), pltpu.roll(t, k, 2))

    def cube(t, k):
        t = t + (pltpu.roll(t, k, 1) + pltpu.roll(t, R - k, 1))
        up = jnp.where(lane >= k, pltpu.roll(t, k, 2), 0.0)
        down = jnp.where(lane < Z - k, pltpu.roll(t, Z - k, 2), 0.0)
        return t + (up + down)

    def mean_shift(i):
        s = dA[pl.ds(2 * i, 2)]
        dd1[pl.ds(i, 1)] = pair_sum(s[0:1] + s[1:2], 1) * 0.125

    loop(n1, mean_shift)

    def diag0(i):
        s = dA[pl.ds(i, 1)]
        wc0[pl.ds(i, 1)] = relax / (CENTER + s)
        dA[pl.ds(i, 1)] = (CENTER + 1.0) + s

    loop(n0, diag0)

    def diag2(i):
        s = dd1[pl.ds(2 * i, 2)]
        s2 = pair_sum(s[0:1] + s[1:2], 2) * 0.125
        wc2[pl.ds(i, 1)] = relax / (CENTER + 16.0 * s2)

    loop(n2, diag2)

    def diag1(i):
        s = dd1[pl.ds(i, 1)]
        wc1[pl.ds(i, 1)] = relax / (CENTER + 4.0 * s)
        dd1[pl.ds(i, 1)] = (CENTER + 1.0) + 4.0 * s

    loop(n1, diag1)

    def scaled(dst, src, wc, count, ch):
        def body(i):
            at = i * ch
            dst[pl.ds(at + 1, ch)] = wc[pl.ds(at, ch)] * src[pl.ds(at, ch)]

        loop(count // ch, body)

    def sweep(dst, src, wg, wc, count, k, ch):
        def body(i):
            at = i * ch
            e = src[pl.ds(at, ch + 2)]
            mid = e[1:ch + 1]
            s = cube(e[0:ch] + mid + e[2:ch + 2], k)
            dst[pl.ds(at + 1, ch)] = (
                KEEP * mid + wg[pl.ds(at + 1, ch)] + wc[pl.ds(at, ch)] * (s - mid)
            )

        loop(count // ch, body)

    def down(dst, src, g, dp, count, k, ch):
        def body(i):
            at = i * ch
            e = src[pl.ds(at, ch + 2)]
            mid = e[1:ch + 1]
            s = cube(e[0:ch] + mid + e[2:ch + 2], k)
            left = g[pl.ds(at, ch)] - dp[pl.ds(at, ch)] * mid + s
            for h in range(ch // 2):
                both = left[2 * h:2 * h + 1] + left[2 * h + 1:2 * h + 2]
                dst[pl.ds(i * (ch // 2) + h, 1)] = 0.5 * pair_sum(both, k)

        loop(count // ch, body)

    def up(dst, src, count):
        def body(i):
            dst[pl.ds(2 * i + 1, 2)] = dst[pl.ds(2 * i + 1, 2)] + src[pl.ds(i + 1, 1)]

        loop(count // 2, body)

    def vcycle(dst, g, scratch):
        g2 = scratch
        scaled(e1, g, wc0, n0, 4)
        sweep(eA, e1, e1, wc0, n0, 1, 4)
        down(g1, eA, g, dA, n0, 1, 4)
        scaled(e1b, g1, wc1, n1, 2)
        sweep(eAb, e1b, e1b, wc1, n1, 2, 2)
        down(g2, eAb, g1, dd1, n1, 2, 2)
        scaled(e1c, g2, wc2, n2, n2)
        sweep(eAc, e1c, e1c, wc2, n2, 4, n2)
        sweep(eBc, eAc, e1c, wc2, n2, 4, n2)
        sweep(eAc, eBc, e1c, wc2, n2, 4, n2)
        up(eAb, eAc, n1)
        sweep(eBb, eAb, e1b, wc1, n1, 2, 2)
        sweep(eAb, eBb, e1b, wc1, n1, 2, 2)
        up(eA, eAb, n0)
        sweep(eB, eA, e1, wc0, n0, 1, 4)
        sweep(dst, eB, e1, wc0, n0, 1, 4)

    for r in range(ROUNDS):
        vcycle(vbox.at[r], g0 if r == 0 else wext.at[r - 1], eBc.at[pl.ds(1, n2)])
        copies = back_copies(r)
        ss, rs = s_sem.at[r], r_sem.at[r]
        start(copies, ss, rs)
        arrive(copies, ss, rs)

        v = vext.at[r]

        def take(i):
            v[pl.ds(2 * i, 2)] = vbox[r, pl.ds(2 * i, 2)]

        loop((n0 + 2) // 2, take)
        for k in range(2):
            s = 0 if k == 0 else X + 1
            v[s:s + 5] = v[s:s + 5] + rx[r, k]
        for k in range(2):
            t = 0 if k == 0 else Y
            v[1:n0 + 1, t:t + 8, :] = v[1:n0 + 1, t:t + 8, :] + ry[r, k]
        for k, (dx, dy) in enumerate(CORNERS):
            s = 0 if dx < 0 else X + 1
            t = 0 if dy < 0 else Y
            v[s:s + 5, t:t + 8, :] = v[s:s + 5, t:t + 8, :] + rc[r, k]

        def trim(i):
            t = v[pl.ds(2 * i, 2)] * in_grid
            if r:
                t = t - THETA * vext[r - 1, pl.ds(2 * i, 2)]
            v[pl.ds(2 * i, 2)] = t

        loop((n0 + 2) // 2, trim)

        @pl.when(ix == 0)
        def _():
            v[0:3] = jnp.zeros((3, R, Z), jnp.float32)

        @pl.when(ix == gx - 1)
        def _():
            v[X + 3:X + 6] = jnp.zeros((3, R, Z), jnp.float32)

        w = wext.at[r]

        def apply(i):
            at = i * 4
            e = v[pl.ds(at, 6)]
            mid = e[1:5]
            s = cube(e[0:4] + mid + e[2:6], 1)
            w[pl.ds(at, 4)] = in_grid * (dA[pl.ds(at, 4)] * mid - s)

        loop(n0 // 4, apply)

        @pl.when(ix == 0)
        def _():
            w[0:2] = jnp.zeros((2, R, Z), jnp.float32)

        @pl.when(ix == gx - 1)
        def _():
            w[X + 2:X + 4] = jnp.zeros((2, R, Z), jnp.float32)

    own = jnp.where(jnp.logical_and(row >= 3, row < Y + 3), 1.0, 0.0).astype(jnp.float32)

    def fold(t):
        t = t.reshape(R // 8, 8, Z)
        return jnp.sum(t, axis=0)

    def dots(i, sums):
        r0 = g0[pl.ds(i + 2, 1)]
        vs = [own * vext[k, pl.ds(i + 3, 1)] for k in range(ROUNDS)]
        ws = [wext[k, pl.ds(i + 2, 1)] for k in range(ROUNDS)]
        terms = [r0 * t for t in vs]
        terms += [vs[a] * ws[b] for a in range(ROUNDS) for b in range(a, ROUNDS)]
        return tuple(s + fold(t) for s, t in zip(sums, terms))

    zero = jnp.zeros((8, Z), jnp.float32)
    sums = lax.fori_loop(0, X, dots, (zero,) * 9)
    line = lax.broadcasted_iota(jnp.int32, (1, Z), 1)
    packed = jnp.zeros((1, Z), jnp.float32)
    for k, s in enumerate(sums):
        total = jnp.sum(jnp.sum(s, axis=0, keepdims=True), axis=1, keepdims=True)
        packed = jnp.where(line == k, total, packed)
    gram[me] = packed

    def gram_copy(d, back):
        other = lax.rem(me + d, n)
        slot = lax.rem(me + n - d, n) if back else me
        return pltpu.make_async_remote_copy(
            src_ref=gram.at[me], dst_ref=gram.at[slot],
            send_sem=gs_sem.at[d], recv_sem=gr_sem.at[slot],
            device_id=(other // gy, lax.rem(other, gy)), device_id_type=MESH,
        )

    @pl.loop(1, n)
    def _(d):
        gram_copy(d, False).start()

    @pl.loop(1, n)
    def _(d):
        gram_copy(d, True).wait_recv()

    total = jnp.sum(gram[...], axis=0)
    b0, b1, b2, g00, g01, g02, g11, g12, g22 = [
        jnp.broadcast_to(
            jnp.sum(jnp.where(line == k, total, 0.0), axis=1, keepdims=True), (1, Z)
        )
        for k in range(9)
    ]
    l1, l2 = g01 / g00, g02 / g00
    d1 = g11 - l1 * g01
    f12 = g12 - l1 * g02
    l3 = f12 / d1
    d2 = g22 - l2 * g02 - l3 * f12
    c1 = b1 - l1 * b0
    c2 = b2 - l2 * b0 - l3 * c1
    y2 = c2 / d2
    y1 = (c1 - f12 * y2) / d1
    y0 = (b0 - g01 * y1 - g02 * y2) / g00
    ys = [jnp.broadcast_to(t, (Y, Z)) for t in (y0, y1, y2)]

    def finish(i):
        x = ys[0] * vext[0, i + 3, 3:Y + 3, :]
        res = rhs[i] - ys[0] * wext[0, i + 2, 3:Y + 3, :]
        for k in range(1, ROUNDS):
            x = x + ys[k] * vext[k, i + 3, 3:Y + 3, :]
            res = res - ys[k] * wext[k, i + 2, 3:Y + 3, :]
        out_x[i] = x
        out_r[i] = res

    loop(X, finish)

    leave(firsts, is_sem, ir_sem)
    for r in range(ROUNDS):
        leave(back_copies(r), s_sem.at[r], r_sem.at[r])

    @pl.loop(1, n)
    def _(d):
        gram_copy(d, False).wait_send()


def on_device(gx, gy, right_side, shift):
    X, Y, Z = right_side.shape
    R = Y + 8
    n0, n1, n2 = X + 4, (X + 4) // 2, (X + 4) // 4
    n = gx * gy

    def field(*lead):
        return pltpu.VMEM(tuple(lead) + (R, Z), jnp.float32)

    scratch = [
        field(n0), field(n0), field(n0), field(n0 + 2), field(n0 + 2), field(n0 + 2),
        field(ROUNDS, n0 + 2), field(ROUNDS, n0 + 2), field(ROUNDS, n0),
        field(n1), field(n1), field(n1), field(n1 + 2), field(n1 + 2), field(n1 + 2),
        field(n2), field(n2 + 2), field(n2 + 2), field(n2 + 2),
        pltpu.VMEM((2, X, 8, Z), jnp.float32),
        pltpu.VMEM((2, 2, 2, Y, Z), jnp.float32),
        pltpu.VMEM((2, X, 8, Z), jnp.float32),
        pltpu.VMEM((4, 2, 8, Z), jnp.float32),
        field(ROUNDS, 2, 5),
        pltpu.VMEM((ROUNDS, 2, n0, 8, Z), jnp.float32),
        pltpu.VMEM((ROUNDS, 4, 5, 8, Z), jnp.float32),
        pltpu.VMEM((n, 1, Z), jnp.float32),
        pltpu.SemaphoreType.DMA((10,)),
        pltpu.SemaphoreType.DMA((10,)),
        pltpu.SemaphoreType.DMA((ROUNDS, 8)),
        pltpu.SemaphoreType.DMA((ROUNDS, 8)),
        pltpu.SemaphoreType.DMA((n,)),
        pltpu.SemaphoreType.DMA((n,)),
    ]
    shape = jax.ShapeDtypeStruct(right_side.shape, jnp.float32)
    return pl.pallas_call(
        functools.partial(kernel, gx, gy, X, Y, Z),
        out_shape=(shape, shape),
        in_specs=[pl.BlockSpec(memory_space=pltpu.VMEM)] * 2,
        out_specs=(pl.BlockSpec(memory_space=pltpu.VMEM),) * 2,
        scratch_shapes=scratch,
        compiler_params=pltpu.CompilerParams(
            collective_id=0, has_side_effects=True, vmem_limit_bytes=40 * 1024 * 1024
        ),
    )(right_side, shift)


def solution(mesh):
    spec = P("gx", "gy", None)
    return jax.shard_map(
        functools.partial(on_device, mesh.shape["gx"], mesh.shape["gy"]),
        mesh=mesh, in_specs=(spec, spec), out_specs=(spec, spec), check_vma=False,
    )
```

```python
import functools

import jax
import jax.numpy as jnp
from jax import lax
from jax.experimental import pallas as pl
from jax.experimental.pallas import tpu as pltpu
from jax.sharding import PartitionSpec as P

MESH = pl.DeviceIdType.MESH
ROUNDS = 3
SWEEPS = 2
BOTTOM = 4
CENTER = 26.0
RELAX = 0.7
KEEP = 1.0 - RELAX
THETA = 1.0
TOP = 8

SIDES = [(-1, 0), (1, 0), (0, -1), (0, 1)]
CORNERS = [(-1, -1), (-1, 1), (1, -1), (1, 1)]


def loop(count, body):
    def step(i, carry):
        body(i)
        return carry

    lax.fori_loop(0, count, step, 0)


def up8(k):
    return (k + 7) // 8 * 8


def kernel(
    gx, gy, X, Y, Z,
    rhs_hbm, shf_hbm, out_x, out_r,
    rhs, shf, g0, dA, wc0, cc0, e1, eA, eB, vbox, vext, wext,
    wc1, cc1, dd1, g1, e1b, eAb, eBb, wc2, cc2, g2, e1c, eAc, eBc,
    pack, in_x, in_y, in_c, ypack, rx, ry, rc, gram,
    ld_sem, is_sem, ir_sem, s_sem, r_sem, gs_sem, gr_sem,
):
    n = gx * gy
    R = Y + 8
    n0, n1, n2 = X + 4, (X + 4) // 2, (X + 4) // 4
    ix, iy = lax.axis_index("gx"), lax.axis_index("gy")
    me = ix * gy + iy
    rows = slice(TOP, TOP + R)

    def there(dx, dy):
        ok = None
        for d, i, c in ((dx, ix, gx), (dy, iy, gy)):
            if d:
                here = (i > 0) if d < 0 else (i < c - 1)
                ok = here if ok is None else jnp.logical_and(ok, here)
        return ok

    loads = [
        pltpu.make_async_copy(src, dst, ld_sem.at[k])
        for k, (src, dst) in enumerate(((rhs_hbm, rhs), (shf_hbm, shf)))
    ]
    for copy in loads:
        copy.start()
    barrier = pltpu.get_barrier_semaphore()

    @pl.loop(1, n)
    def _(d):
        other = lax.rem(me + d, n)
        pl.semaphore_signal(
            barrier, inc=1, device_id=(other // gy, lax.rem(other, gy)), device_id_type=MESH
        )

    for copy in loads:
        copy.wait()

    for side, at in ((0, 0), (1, Y - 2)):
        for p in range(X // 2):
            for q in range(2):
                pack[side, p, 4 * q:4 * q + 2, :] = rhs[2 * p + q, at:at + 2, :]
                pack[side, p, 4 * q + 2:4 * q + 4, :] = shf[2 * p + q, at:at + 2, :]

    pl.semaphore_wait(barrier, n - 1)

    def remote(item, ss, rs, dx, dy):
        return pltpu.make_async_remote_copy(
            src_ref=item[2], dst_ref=item[3], send_sem=ss.at[item[4]], recv_sem=rs.at[item[5]],
            device_id=(ix + dx, iy + dy), device_id_type=MESH,
        )

    def first_copies():
        result = []
        for k, (dx, dy) in enumerate(SIDES):
            if dx:
                at = 0 if dx < 0 else X - 2
                for a, ref in enumerate((rhs, shf)):
                    result.append((dx, dy, ref.at[pl.ds(at, 2)], in_x.at[k ^ 1, a],
                                   2 * k + a, 2 * (k ^ 1) + a))
            else:
                result.append((dx, dy, pack.at[k - 2], in_y.at[(k - 2) ^ 1],
                               2 + k, 2 + (k ^ 1)))
        for k, (dx, dy) in enumerate(CORNERS):
            at = 0 if dx < 0 else X // 2 - 1
            result.append((dx, dy, pack.at[0 if dy < 0 else 1, at], in_c.at[3 - k],
                           6 + k, 6 + 3 - k))
        return result

    def depth(r):
        return 5 if r + 1 < ROUNDS else 3

    def corner_rows(r, dx):
        d = depth(r)
        if dx < 0:
            return 0, up8(d * d), 0
        base = (n0 - d) * d
        return base // 8 * 8, up8(n0 * d), base % 8

    def back_copies(r):
        result = []
        d = depth(r)
        for k, (dx, dy) in enumerate(SIDES):
            if dx:
                at = 1 if dx < 0 else X + 5 - d
                src = vbox.at[r, pl.ds(at, d), pl.ds(TOP, R)]
                result.append((dx, dy, src, rx.at[r, k ^ 1, pl.ds(0, d)], k, k ^ 1))
            else:
                tall = up8(n0 * d)
                result.append((dx, dy, ypack.at[r, k - 2, pl.ds(0, tall)],
                               ry.at[r, (k - 2) ^ 1, pl.ds(0, tall)], k, k ^ 1))
        for k, (dx, dy) in enumerate(CORNERS):
            lo, hi, _ = corner_rows(r, dx)
            src = ypack.at[r, 0 if dy < 0 else 1, pl.ds(lo, hi - lo)]
            result.append((dx, dy, src, rc.at[r, 3 - k, pl.ds(0, hi - lo)], 4 + k, 4 + 3 - k))
        return result

    def start(copies, ss, rs):
        for item in copies[::-1]:
            dx, dy = item[:2]

            @pl.when(there(dx, dy))
            def _(item=item, dx=dx, dy=dy):
                remote(item, ss, rs, dx, dy).start()

    def arrive(copies, ss, rs, use):
        for item in copies:
            dx, dy = -item[0], -item[1]

            @pl.when(there(dx, dy))
            def _(item=item, dx=dx, dy=dy):
                remote(item, ss, rs, dx, dy).wait_recv()
                use(dx, dy, item[3], item[5])

    def leave(copies, ss, rs):
        for item in copies:
            dx, dy = item[:2]

            @pl.when(there(dx, dy))
            def _(item=item, dx=dx, dy=dy):
                remote(item, ss, rs, dx, dy).wait_send()

    firsts = first_copies()
    start(firsts, is_sem, ir_sem)

    for ref in (eA, eB, e1, vbox, vext, g0, dA, eAb, eBb, e1b, eAc, eBc, e1c):
        lead = ref.shape[:-2]

        def clear(i, ref=ref, lead=lead):
            at = (i,) if len(lead) == 1 else (i // lead[1], lax.rem(i, lead[1]))
            ref[at] = jnp.zeros(ref.shape[-2:], jnp.float32)

        loop(lead[0] if len(lead) == 1 else lead[0] * lead[1], clear)

    row = lax.broadcasted_iota(jnp.int32, (1, R, Z), 1)
    lane = lax.broadcasted_iota(jnp.int32, (1, R, Z), 2)

    g0[2:X + 2, 3:Y + 3, :] = rhs[...]
    dA[2:X + 2, 3:Y + 3, :] = shf[...]

    def use_first(dx, dy, got, slot):
        s = 0 if dx < 0 else X + 2
        t = 1 if dy < 0 else Y + 3
        if dy == 0:
            (g0, dA)[slot % 2][s:s + 2, 3:Y + 3, :] = got[...]
            return
        for a, ref in enumerate((g0, dA)):
            if dx == 0:
                for i in range(X):
                    q = 4 * (i % 2) + 2 * a
                    ref[2 + i, t:t + 2, :] = got[i // 2, q:q + 2, :]
            else:
                for q in range(2):
                    p = 4 * q + 2 * a
                    ref[s + q, t:t + 2, :] = got[p:p + 2, :]

    arrive(firsts, is_sem, ir_sem, use_first)

    in_box = jnp.logical_and(row >= 1, row <= Y + 4)
    relax = jnp.where(in_box, RELAX, 0.0).astype(jnp.float32)
    at_y = iy * Y + row - 3
    in_grid = jnp.where(
        jnp.logical_and(at_y >= 0, at_y < gy * Y), 1.0, 0.0
    ).astype(jnp.float32)

    def pair_sum(t, k):
        first = lax.rem(jnp.maximum(row - 1, 0) // k, 2) == 0
        t = t + jnp.where(first, pltpu.roll(t, R - k, 1), pltpu.roll(t, k, 1))
        low = lax.rem(lane // k, 2) == 0
        return t + jnp.where(low, pltpu.roll(t, Z - k, 2), pltpu.roll(t, k, 2))

    def cube(src, at, ch, k):
        got = src[pl.ds(at, ch + 2), rows, :]
        t = got + (
            src[pl.ds(at, ch + 2), TOP - k:TOP - k + R, :]
            + src[pl.ds(at, ch + 2), TOP + k:TOP + k + R, :]
        )
        t = t[0:ch] + t[1:ch + 1] + t[2:ch + 2]
        up = jnp.where(lane >= k, pltpu.roll(t, k, 2), 0.0)
        down = jnp.where(lane < Z - k, pltpu.roll(t, Z - k, 2), 0.0)
        return got[1:ch + 1], t + (up + down)

    def mean_shift(i):
        s = dA[pl.ds(2 * i, 2)]
        dd1[pl.ds(i, 1)] = pair_sum(s[0:1] + s[1:2], 1) * 0.125

    loop(n1, mean_shift)

    def weights(wc, cc, dp, count, values):
        def body(i):
            d = CENTER + values(i)
            w = relax / d
            wc[pl.ds(i, 1)] = w
            cc[pl.ds(i, 1)] = KEEP - w
            if dp is not None:
                dp[pl.ds(i, 1)] = d + 1.0

        loop(count, body)

    def mean_second(i):
        s = dd1[pl.ds(2 * i, 2)]
        return 16.0 * (pair_sum(s[0:1] + s[1:2], 2) * 0.125)

    weights(wc0, cc0, dA, n0, lambda i: dA[pl.ds(i, 1)])
    weights(wc2, cc2, None, n2, mean_second)
    weights(wc1, cc1, dd1, n1, lambda i: 4.0 * dd1[pl.ds(i, 1)])

    def scaled(dst, src, wc, count, ch):
        def body(i):
            at = i * ch
            dst[pl.ds(at + 1, ch), rows, :] = wc[pl.ds(at, ch)] * src[pl.ds(at, ch)]

        loop(count // ch, body)

    def sweep(dst, src, wg, wc, cc, count, k, ch):
        def body(i):
            at = i * ch
            mid, s = cube(src, at, ch, k)
            base = mid if wg is src else wg[pl.ds(at + 1, ch), rows, :]
            dst[pl.ds(at + 1, ch), rows, :] = (
                cc[pl.ds(at, ch)] * mid + base + wc[pl.ds(at, ch)] * s
            )

        loop(count // ch, body)

    def down(dst, src, g, dp, count, k, ch):
        def body(i):
            at = i * ch
            mid, s = cube(src, at, ch, k)
            left = g[pl.ds(at, ch)] - dp[pl.ds(at, ch)] * mid + s
            both = [left[2 * h:2 * h + 1] + left[2 * h + 1:2 * h + 2] for h in range(ch // 2)]
            both = jnp.concatenate(both, axis=0)
            dst[pl.ds(i * (ch // 2), ch // 2)] = 0.5 * pair_sum(both, k)

        loop(count // ch, body)

    def up(dst, src, count):
        def body(i):
            dst[pl.ds(2 * i + 1, 2), rows, :] = (
                dst[pl.ds(2 * i + 1, 2), rows, :] + src[pl.ds(i + 1, 1), rows, :]
            )

        loop(count // 2, body)

    h0 = n0 // 2

    def vcycle(dst, g):
        sweep(eA, e1, e1, wc0, cc0, n0, 1, h0)
        down(g1, eA, g, dA, n0, 1, h0)
        scaled(e1b, g1, wc1, n1, n1)
        sweep(eAb, e1b, e1b, wc1, cc1, n1, 2, n1)
        down(g2, eAb, g1, dd1, n1, 2, n1)
        scaled(e1c, g2, wc2, n2, n2)
        sweep(eAc, e1c, e1c, wc2, cc2, n2, 4, n2)
        for turn in range(BOTTOM - 2):
            a, b = (eBc, eAc) if turn % 2 == 0 else (eAc, eBc)
            sweep(a, b, e1c, wc2, cc2, n2, 4, n2)
        up(eAb, eAc, n1)
        sweep(eBb, eAb, e1b, wc1, cc1, n1, 2, n1)
        sweep(eAb, eBb, e1b, wc1, cc1, n1, 2, n1)
        up(eA, eAb, n0)
        sweep(eB, eA, e1, wc0, cc0, n0, 1, h0)
        sweep(dst, eB, e1, wc0, cc0, n0, 1, h0)

    own = jnp.where(jnp.logical_and(row >= 3, row < Y + 3), 1.0, 0.0).astype(jnp.float32)

    def dots(r):
        ch = 4

        def body(i, sums):
            w = own * wext[r, pl.ds(ch * i + 2, ch)]
            terms = [own * g0[pl.ds(ch * i + 2, ch)] * vext[r, pl.ds(ch * i + 3, ch), rows, :]]
            terms += [vext[a, pl.ds(ch * i + 3, ch), rows, :] * w for a in range(r + 1)]
            return tuple(
                s + jnp.sum(t.reshape(ch * R // 8, 8, Z), axis=0) for s, t in zip(sums, terms)
            )

        zero = jnp.zeros((8, Z), jnp.float32)
        return lax.fori_loop(0, X // ch, body, (zero,) * (r + 2))

    scaled(e1, g0, wc0, n0, 4)
    sums = []
    for r in range(ROUNDS):
        vcycle(vbox.at[r], g0 if r == 0 else wext.at[r - 1])
        d = depth(r)
        for i in range(n0):
            ypack[r, 0, d * i:d * i + d, :] = vbox[r, i + 1, TOP + 1:TOP + 1 + d, :]
            ypack[r, 1, d * i:d * i + d, :] = vbox[r, i + 1, TOP + Y + 5 - d:TOP + Y + 5, :]
        copies = back_copies(r)
        ss, rs = s_sem.at[r], r_sem.at[r]
        start(copies, ss, rs)

        v = vext.at[r]

        def take(i):
            at = pl.ds(2 * i, 2)
            t = vbox[r, at, rows, :] * in_grid
            if r:
                t = t - THETA * vext[r - 1, at, rows, :]
            v[at, rows, :] = t

        loop((n0 + 2) // 2, take)
        if r:
            sums.append(dots(r - 1))

        def use_back(dx, dy, got, slot):
            s = 5 - d if dx < 0 else X + 1
            t = TOP + 5 - d if dy < 0 else TOP + Y + 1
            if dy == 0:
                v[s:s + d, rows, :] = v[s:s + d, rows, :] + got[...] * in_grid
                return
            skip = 0 if dx == 0 else corner_rows(r, -dx)[2]
            if dx == 0:
                s = 1
            for j in range(n0 if dx == 0 else d):
                v[s + j, t:t + d, :] = (
                    v[s + j, t:t + d, :] + got[skip + d * j:skip + d * j + d, :]
                )

        arrive(copies, ss, rs, use_back)

        @pl.when(ix == 0)
        def _():
            v[0:3, rows, :] = jnp.zeros((3, R, Z), jnp.float32)

        @pl.when(ix == gx - 1)
        def _():
            v[X + 3:X + 6, rows, :] = jnp.zeros((3, R, Z), jnp.float32)

        w = wext.at[r]
        last = r + 1 == ROUNDS

        def apply(i):
            ch = X // 2 if last else h0
            at = i * ch + (2 if last else 0)
            mid, s = cube(v, at, ch, 1)
            t = in_grid * (dA[pl.ds(at, ch)] * mid - s)
            w[pl.ds(at, ch)] = t
            if not last:
                e1[pl.ds(at + 1, ch), rows, :] = wc0[pl.ds(at, ch)] * t

        loop(2, apply)

        if not last:
            for edge, at in ((0, 0), (gx - 1, X + 2)):
                @pl.when(ix == edge)
                def _(at=at):
                    w[at:at + 2] = jnp.zeros((2, R, Z), jnp.float32)
                    e1[at + 1:at + 3, rows, :] = jnp.zeros((2, R, Z), jnp.float32)

    sums.append(dots(ROUNDS - 1))
    flat = [t for group in sums for t in group]
    line = lax.broadcasted_iota(jnp.int32, (1, Z), 1)
    packed = jnp.zeros((1, Z), jnp.float32)
    for k, s in enumerate(flat):
        total = jnp.sum(jnp.sum(s, axis=0, keepdims=True), axis=1, keepdims=True)
        packed = jnp.where(line == k, total, packed)
    gram[me] = packed

    def gram_copy(d, back):
        other = lax.rem(me + d, n)
        slot = lax.rem(me + n - d, n) if back else me
        return pltpu.make_async_remote_copy(
            src_ref=gram.at[me], dst_ref=gram.at[slot],
            send_sem=gs_sem.at[d], recv_sem=gr_sem.at[slot],
            device_id=(other // gy, lax.rem(other, gy)), device_id_type=MESH,
        )

    @pl.loop(1, n)
    def _(d):
        gram_copy(d, False).start()

    @pl.loop(1, n)
    def _(d):
        gram_copy(d, True).wait_recv()

    total = jnp.sum(gram[...], axis=0)
    b0, g00, b1, g01, g11, b2, g02, g12, g22 = [
        jnp.broadcast_to(
            jnp.sum(jnp.where(line == k, total, 0.0), axis=1, keepdims=True), (1, Z)
        )
        for k in range(9)
    ]
    l1, l2 = g01 / g00, g02 / g00
    d1 = g11 - l1 * g01
    f12 = g12 - l1 * g02
    l3 = f12 / d1
    d2 = g22 - l2 * g02 - l3 * f12
    c1 = b1 - l1 * b0
    c2 = b2 - l2 * b0 - l3 * c1
    y2 = c2 / d2
    y1 = (c1 - f12 * y2) / d1
    y0 = (b0 - g01 * y1 - g02 * y2) / g00
    ys = [jnp.broadcast_to(t, (Y, Z)) for t in (y0, y1, y2)]

    def finish(i):
        x = ys[0] * vext[0, i + 3, TOP + 3:TOP + Y + 3, :]
        res = rhs[i] - ys[0] * wext[0, i + 2, 3:Y + 3, :]
        for k in range(1, ROUNDS):
            x = x + ys[k] * vext[k, i + 3, TOP + 3:TOP + Y + 3, :]
            res = res - ys[k] * wext[k, i + 2, 3:Y + 3, :]
        out_x[i] = x
        out_r[i] = res

    loop(X, finish)

    leave(firsts, is_sem, ir_sem)
    for r in range(ROUNDS):
        leave(back_copies(r), s_sem.at[r], r_sem.at[r])

    @pl.loop(1, n)
    def _(d):
        gram_copy(d, False).wait_send()


def on_device(gx, gy, right_side, shift):
    X, Y, Z = right_side.shape
    R = Y + 8
    n0, n1, n2 = X + 4, (X + 4) // 2, (X + 4) // 4
    n = gx * gy

    def field(*lead):
        return pltpu.VMEM(tuple(lead) + (R, Z), jnp.float32)

    def tall(*lead):
        return pltpu.VMEM(tuple(lead) + (R + 2 * TOP, Z), jnp.float32)

    def plain(*shape):
        return pltpu.VMEM(tuple(shape) + (Z,), jnp.float32)

    packed = up8(n0 * 5)
    scratch = [
        plain(X, Y), plain(X, Y),
        field(n0), field(n0), field(n0), field(n0), tall(n0 + 2), tall(n0 + 2), tall(n0 + 2),
        tall(ROUNDS, n0 + 2), tall(ROUNDS, n0 + 2), field(ROUNDS, n0),
        field(n1), field(n1), field(n1), field(n1), tall(n1 + 2), tall(n1 + 2), tall(n1 + 2),
        field(n2), field(n2), field(n2), tall(n2 + 2), tall(n2 + 2), tall(n2 + 2),
        plain(2, X // 2, 8), plain(2, 2, 2, Y), plain(2, X // 2, 8), plain(4, 8),
        plain(ROUNDS, 2, packed), field(ROUNDS, 2, 5), plain(ROUNDS, 2, packed),
        plain(ROUNDS, 4, 32), plain(n, 1),
        pltpu.SemaphoreType.DMA((2,)),
        pltpu.SemaphoreType.DMA((10,)),
        pltpu.SemaphoreType.DMA((10,)),
        pltpu.SemaphoreType.DMA((ROUNDS, 8)),
        pltpu.SemaphoreType.DMA((ROUNDS, 8)),
        pltpu.SemaphoreType.DMA((n,)),
        pltpu.SemaphoreType.DMA((n,)),
    ]
    shape = jax.ShapeDtypeStruct(right_side.shape, jnp.float32)
    return pl.pallas_call(
        functools.partial(kernel, gx, gy, X, Y, Z),
        out_shape=(shape, shape),
        in_specs=[pl.BlockSpec(memory_space=pltpu.HBM)] * 2,
        out_specs=(pl.BlockSpec(memory_space=pltpu.VMEM),) * 2,
        scratch_shapes=scratch,
        compiler_params=pltpu.CompilerParams(
            collective_id=0, has_side_effects=True, vmem_limit_bytes=40 * 1024 * 1024
        ),
    )(right_side, shift)


def solution(mesh):
    spec = P("gx", "gy", None)
    return jax.shard_map(
        functools.partial(on_device, mesh.shape["gx"], mesh.shape["gy"]),
        mesh=mesh, in_specs=(spec, spec), out_specs=(spec, spec), check_vma=False,
    )
```

```python
import functools

import jax
import jax.numpy as jnp
from jax import lax
from jax.experimental import pallas as pl
from jax.experimental.pallas import tpu as pltpu
from jax.sharding import PartitionSpec as P

MESH = pl.DeviceIdType.MESH
ROUNDS = 3
SWEEPS = 2
BOTTOM = 4
CENTER = 26.0
RELAX = 0.7
KEEP = 1.0 - RELAX
THETA = 1.0
TOP = 8
VMEM_GRANT = 41943040

SIDES = [(-1, 0), (1, 0), (0, -1), (0, 1)]
CORNERS = [(-1, -1), (-1, 1), (1, -1), (1, 1)]


def loop(count, body):
    def step(i, carry):
        body(i)
        return carry

    lax.fori_loop(0, count, step, 0)


def up8(k):
    return (k + 7) // 8 * 8


def kernel(
    gx, gy, X, Y, Z,
    rhs_hbm, shf_hbm, out_x, out_r,
    rhs, shf, g0, dA, wc0, cc0, e1, eA, eB, vbox, vext, wext,
    wc1, cc1, dd1, g1, e1b, eAb, eBb, wc2, cc2, g2, e1c, eAc, eBc,
    pack, in_x, in_y, in_c, ypack, rx, ry, rc, gram,
    ld_sem, is_sem, ir_sem, s_sem, r_sem, gs_sem, gr_sem,
):
    n = gx * gy
    R = Y + 8
    n0, n1, n2 = X + 4, (X + 4) // 2, (X + 4) // 4
    ix, iy = lax.axis_index("gx"), lax.axis_index("gy")
    me = ix * gy + iy
    rows = slice(TOP, TOP + R)

    def there(dx, dy):
        ok = None
        for d, i, c in ((dx, ix, gx), (dy, iy, gy)):
            if d:
                here = (i > 0) if d < 0 else (i < c - 1)
                ok = here if ok is None else jnp.logical_and(ok, here)
        return ok

    loads = [
        pltpu.make_async_copy(src, dst, ld_sem.at[k])
        for k, (src, dst) in enumerate(((rhs_hbm, rhs), (shf_hbm, shf)))
    ]
    for copy in loads:
        copy.start()
    barrier = pltpu.get_barrier_semaphore()

    xs = [ix] + [jnp.where(ix + k < gx, ix + k, ix + k - gx) for k in range(1, gx)]
    ys_at = [iy] + [jnp.where(iy + k < gy, iy + k, iy + k - gy) for k in range(1, gy)]
    others = [(a, b) for a in range(gx) for b in range(gy)][1:]
    for a, b in others:
        pl.semaphore_signal(
            barrier, inc=1, device_id=(xs[a], ys_at[b]), device_id_type=MESH
        )

    for ref in (eA, eB, e1, vbox, vext, g0, dA, eAb, eBb, e1b, eAc, eBc, e1c):
        lead = ref.shape[:-2]

        def clear(i, ref=ref, lead=lead):
            at = (i,) if len(lead) == 1 else (i // lead[1], lax.rem(i, lead[1]))
            ref[at] = jnp.zeros(ref.shape[-2:], jnp.float32)

        loop(lead[0] if len(lead) == 1 else lead[0] * lead[1], clear)

    for copy in loads:
        copy.wait()

    for side, at in ((0, 0), (1, Y - 2)):
        for p in range(X // 2):
            for q in range(2):
                pack[side, p, 4 * q:4 * q + 2, :] = rhs[2 * p + q, at:at + 2, :]
                pack[side, p, 4 * q + 2:4 * q + 4, :] = shf[2 * p + q, at:at + 2, :]

    g0[2:X + 2, 3:Y + 3, :] = rhs[...]
    dA[2:X + 2, 3:Y + 3, :] = shf[...]

    pl.semaphore_wait(barrier, n - 1)

    def remote(item, ss, rs, dx, dy):
        return pltpu.make_async_remote_copy(
            src_ref=item[2], dst_ref=item[3], send_sem=ss.at[item[4]], recv_sem=rs.at[item[5]],
            device_id=(ix + dx, iy + dy), device_id_type=MESH,
        )

    def first_copies():
        result = []
        for k, (dx, dy) in enumerate(SIDES):
            if dx:
                at = 0 if dx < 0 else X - 2
                for a, ref in enumerate((rhs, shf)):
                    result.append((dx, dy, ref.at[pl.ds(at, 2)], in_x.at[k ^ 1, a],
                                   2 * k + a, 2 * (k ^ 1) + a))
            else:
                result.append((dx, dy, pack.at[k - 2], in_y.at[(k - 2) ^ 1],
                               2 + k, 2 + (k ^ 1)))
        for k, (dx, dy) in enumerate(CORNERS):
            at = 0 if dx < 0 else X // 2 - 1
            result.append((dx, dy, pack.at[0 if dy < 0 else 1, at], in_c.at[3 - k],
                           6 + k, 6 + 3 - k))
        return result

    def depth(r):
        return 5 if r + 1 < ROUNDS else 3

    def corner_rows(r, dx):
        d = depth(r)
        if dx < 0:
            return 0, up8(d * d), 0
        base = (n0 - d) * d
        return base // 8 * 8, up8(n0 * d), base % 8

    def back_copies(r):
        result = []
        d = depth(r)
        for k, (dx, dy) in enumerate(SIDES):
            if dx:
                at = 1 if dx < 0 else X + 5 - d
                src = vbox.at[r, pl.ds(at, d), pl.ds(TOP, R)]
                result.append((dx, dy, src, rx.at[r, k ^ 1, pl.ds(0, d)], k, k ^ 1))
            else:
                tall = up8(n0 * d)
                result.append((dx, dy, ypack.at[r, k - 2, pl.ds(0, tall)],
                               ry.at[r, (k - 2) ^ 1, pl.ds(0, tall)], k, k ^ 1))
        for k, (dx, dy) in enumerate(CORNERS):
            lo, hi, _ = corner_rows(r, dx)
            src = ypack.at[r, 0 if dy < 0 else 1, pl.ds(lo, hi - lo)]
            result.append((dx, dy, src, rc.at[r, 3 - k, pl.ds(0, hi - lo)], 4 + k, 4 + 3 - k))
        return result

    def start(copies, ss, rs):
        for item in copies[::-1]:
            dx, dy = item[:2]

            @pl.when(there(dx, dy))
            def _(item=item, dx=dx, dy=dy):
                remote(item, ss, rs, dx, dy).start()

    def arrive(copies, ss, rs, use):
        for item in copies:
            dx, dy = -item[0], -item[1]

            @pl.when(there(dx, dy))
            def _(item=item, dx=dx, dy=dy):
                remote(item, ss, rs, dx, dy).wait_recv()
                use(dx, dy, item[3], item[5])

    def leave(copies, ss, rs):
        for item in copies:
            dx, dy = item[:2]

            @pl.when(there(dx, dy))
            def _(item=item, dx=dx, dy=dy):
                remote(item, ss, rs, dx, dy).wait_send()

    firsts = first_copies()
    start(firsts, is_sem, ir_sem)

    row = lax.broadcasted_iota(jnp.int32, (1, R, Z), 1)
    lane = lax.broadcasted_iota(jnp.int32, (1, R, Z), 2)
    flat_lane = lax.broadcasted_iota(jnp.int32, (R, Z), 1)

    def use_first(dx, dy, got, slot):
        s = 0 if dx < 0 else X + 2
        t = 1 if dy < 0 else Y + 3
        if dy == 0:
            (g0, dA)[slot % 2][s:s + 2, 3:Y + 3, :] = got[...]
            return
        for a, ref in enumerate((g0, dA)):
            if dx == 0:
                for i in range(X):
                    q = 4 * (i % 2) + 2 * a
                    ref[2 + i, t:t + 2, :] = got[i // 2, q:q + 2, :]
            else:
                for q in range(2):
                    p = 4 * q + 2 * a
                    ref[s + q, t:t + 2, :] = got[p:p + 2, :]

    arrive(firsts, is_sem, ir_sem, use_first)

    in_box = jnp.logical_and(row >= 1, row <= Y + 4)
    relax = jnp.where(in_box, RELAX, 0.0).astype(jnp.float32)
    at_y = iy * Y + row - 3
    in_grid = jnp.where(
        jnp.logical_and(at_y >= 0, at_y < gy * Y), 1.0, 0.0
    ).astype(jnp.float32)

    def pair_sum(t, k):
        first = lax.rem(jnp.maximum(row - 1, 0) // k, 2) == 0
        t = t + jnp.where(first, pltpu.roll(t, R - k, 1), pltpu.roll(t, k, 1))
        low = lax.rem(lane // k, 2) == 0
        return t + jnp.where(low, pltpu.roll(t, Z - k, 2), pltpu.roll(t, k, 2))

    def cube(src, at, ch, k):
        last = []
        for j in range(ch + 2):
            got = src[at + j, rows, :]
            t = got + (src[at + j, TOP - k:TOP - k + R, :] + src[at + j, TOP + k:TOP + k + R, :])
            last.append((got, t))
            if j >= 2:
                t = last[0][1] + last[1][1] + last[2][1]
                up = jnp.where(flat_lane >= k, pltpu.roll(t, k, 1), 0.0)
                down = jnp.where(flat_lane < Z - k, pltpu.roll(t, Z - k, 1), 0.0)
                yield j - 2, last[1][0], t + (up + down)
                last = last[1:]

    def mean_shift(i):
        for j in range(5):
            s = dA[pl.ds(10 * i + 2 * j, 2)]
            dd1[pl.ds(5 * i + j, 1)] = pair_sum(s[0:1] + s[1:2], 1) * 0.125

    loop(n1 // 5, mean_shift)

    def weights(wc, cc, dp, count, values):
        def body(i):
            for j in range(5):
                at = pl.ds(5 * i + j, 1)
                d = CENTER + values(5 * i + j)
                w = relax / d
                wc[at] = w
                cc[at] = KEEP - w
                if dp is not None:
                    dp[at] = d + 1.0

        loop(count // 5, body)

    def mean_second(i):
        s = dd1[pl.ds(2 * i, 2)]
        return 16.0 * (pair_sum(s[0:1] + s[1:2], 2) * 0.125)

    weights(wc0, cc0, dA, n0, lambda i: dA[pl.ds(i, 1)])
    weights(wc2, cc2, None, n2, mean_second)
    weights(wc1, cc1, dd1, n1, lambda i: 4.0 * dd1[pl.ds(i, 1)])

    def scaled(dst, src, wc, count, ch):
        def body(i):
            at = i * ch
            dst[pl.ds(at + 1, ch), rows, :] = wc[pl.ds(at, ch)] * src[pl.ds(at, ch)]

        loop(count // ch, body)

    def sweep(dst, src, wg, wc, cc, count, k, ch):
        def body(i):
            at = i * ch
            for j, mid, s in cube(src, at, ch, k):
                base = mid if wg is src else wg[at + j + 1, rows, :]
                dst[at + j + 1, rows, :] = cc[at + j] * mid + base + wc[at + j] * s

        loop(count // ch, body)

    def down(dst, src, g, dp, count, k, ch):
        def body(i):
            at = i * ch
            for j, mid, s in cube(src, at, ch, k):
                left = g[at + j] - dp[at + j] * mid + s
                if j % 2:
                    dst[i * (ch // 2) + j // 2] = 0.5 * pair_sum((held + left)[None], k)[0]
                held = left

        loop(count // ch, body)

    def up(dst, src, count):
        def body(i):
            dst[pl.ds(2 * i + 1, 2), rows, :] = (
                dst[pl.ds(2 * i + 1, 2), rows, :] + src[pl.ds(i + 1, 1), rows, :]
            )

        loop(count // 2, body)

    h0 = n0 // 2

    def vcycle(dst, g):
        sweep(eA, e1, e1, wc0, cc0, n0, 1, h0)
        down(g1, eA, g, dA, n0, 1, h0)
        scaled(e1b, g1, wc1, n1, n1)
        sweep(eAb, e1b, e1b, wc1, cc1, n1, 2, n1)
        down(g2, eAb, g1, dd1, n1, 2, n1)
        scaled(e1c, g2, wc2, n2, n2)
        sweep(eAc, e1c, e1c, wc2, cc2, n2, 4, n2)
        for turn in range(BOTTOM - 2):
            a, b = (eBc, eAc) if turn % 2 == 0 else (eAc, eBc)
            sweep(a, b, e1c, wc2, cc2, n2, 4, n2)
        up(eAb, eAc, n1)
        sweep(eBb, eAb, e1b, wc1, cc1, n1, 2, n1)
        sweep(eAb, eBb, e1b, wc1, cc1, n1, 2, n1)
        up(eA, eAb, n0)
        sweep(eB, eA, e1, wc0, cc0, n0, 1, h0)
        sweep(dst, eB, e1, wc0, cc0, n0, 1, h0)

    own = jnp.where(jnp.logical_and(row >= 3, row < Y + 3), 1.0, 0.0).astype(jnp.float32)

    def dots(r):
        ch = 4

        def body(i, sums):
            w = own * wext[r, pl.ds(ch * i + 2, ch)]
            terms = [own * g0[pl.ds(ch * i + 2, ch)] * vext[r, pl.ds(ch * i + 3, ch), rows, :]]
            terms += [vext[a, pl.ds(ch * i + 3, ch), rows, :] * w for a in range(r + 1)]
            return tuple(
                s + jnp.sum(t.reshape(ch * R // 8, 8, Z), axis=0) for s, t in zip(sums, terms)
            )

        zero = jnp.zeros((8, Z), jnp.float32)
        return lax.fori_loop(0, X // ch, body, (zero,) * (r + 2))

    scaled(e1, g0, wc0, n0, 4)
    sums = []
    for r in range(ROUNDS):
        vcycle(vbox.at[r], g0 if r == 0 else wext.at[r - 1])
        d = depth(r)
        for i in range(n0):
            ypack[r, 0, d * i:d * i + d, :] = vbox[r, i + 1, TOP + 1:TOP + 1 + d, :]
            ypack[r, 1, d * i:d * i + d, :] = vbox[r, i + 1, TOP + Y + 5 - d:TOP + Y + 5, :]
        copies = back_copies(r)
        ss, rs = s_sem.at[r], r_sem.at[r]
        start(copies, ss, rs)

        v = vext.at[r]

        def take(i):
            at = pl.ds(2 * i, 2)
            t = vbox[r, at, rows, :] * in_grid
            if r:
                t = t - THETA * vext[r - 1, at, rows, :]
            v[at, rows, :] = t

        loop((n0 + 2) // 2, take)
        if r:
            sums.append(dots(r - 1))

        def use_back(dx, dy, got, slot):
            s = 5 - d if dx < 0 else X + 1
            t = TOP + 5 - d if dy < 0 else TOP + Y + 1
            if dy == 0:
                v[s:s + d, rows, :] = v[s:s + d, rows, :] + got[...] * in_grid
                return
            skip = 0 if dx == 0 else corner_rows(r, -dx)[2]
            if dx == 0:
                s = 1
            for j in range(n0 if dx == 0 else d):
                v[s + j, t:t + d, :] = (
                    v[s + j, t:t + d, :] + got[skip + d * j:skip + d * j + d, :]
                )

        arrive(copies, ss, rs, use_back)

        @pl.when(ix == 0)
        def _():
            v[0:3, rows, :] = jnp.zeros((3, R, Z), jnp.float32)

        @pl.when(ix == gx - 1)
        def _():
            v[X + 3:X + 6, rows, :] = jnp.zeros((3, R, Z), jnp.float32)

        w = wext.at[r]
        last = r + 1 == ROUNDS

        def apply(i):
            ch = X // 2 if last else h0
            at = i * ch + (2 if last else 0)
            for j, mid, s in cube(v, at, ch, 1):
                t = in_grid[0] * (dA[at + j] * mid - s)
                w[at + j] = t
                if not last:
                    e1[at + j + 1, rows, :] = wc0[at + j] * t

        loop(2, apply)

        if not last:
            for edge, at in ((0, 0), (gx - 1, X + 2)):
                @pl.when(ix == edge)
                def _(at=at):
                    w[at:at + 2] = jnp.zeros((2, R, Z), jnp.float32)
                    e1[at + 1:at + 3, rows, :] = jnp.zeros((2, R, Z), jnp.float32)

    sums.append(dots(ROUNDS - 1))
    flat = [t for group in sums for t in group]
    line = lax.broadcasted_iota(jnp.int32, (1, Z), 1)
    packed = jnp.zeros((1, Z), jnp.float32)
    for k, s in enumerate(flat):
        total = jnp.sum(jnp.sum(s, axis=0, keepdims=True), axis=1, keepdims=True)
        packed = jnp.where(line == k, total, packed)
    gram[me] = packed

    def gram_copy(k, back):
        a, b = others[k]
        slot = me
        if back:
            slot = xs[(gx - a) % gx] * gy + ys_at[(gy - b) % gy]
        return pltpu.make_async_remote_copy(
            src_ref=gram.at[me], dst_ref=gram.at[slot],
            send_sem=gs_sem.at[k], recv_sem=gr_sem.at[slot],
            device_id=(xs[a], ys_at[b]), device_id_type=MESH,
        )

    for k in range(n - 1)[::-1]:
        gram_copy(k, False).start()
    for k in range(n - 1):
        gram_copy(k, True).wait_recv()

    total = jnp.sum(gram[...], axis=0)
    b0, g00, b1, g01, g11, b2, g02, g12, g22 = [
        jnp.broadcast_to(
            jnp.sum(jnp.where(line == k, total, 0.0), axis=1, keepdims=True), (1, Z)
        )
        for k in range(9)
    ]
    l1, l2 = g01 / g00, g02 / g00
    d1 = g11 - l1 * g01
    f12 = g12 - l1 * g02
    l3 = f12 / d1
    d2 = g22 - l2 * g02 - l3 * f12
    c1 = b1 - l1 * b0
    c2 = b2 - l2 * b0 - l3 * c1
    y2 = c2 / d2
    y1 = (c1 - f12 * y2) / d1
    y0 = (b0 - g01 * y1 - g02 * y2) / g00
    ys = [jnp.broadcast_to(t, (Y, Z)) for t in (y0, y1, y2)]

    def finish(i):
        for j in range(4):
            p = 4 * i + j
            x = ys[0] * vext[0, p + 3, TOP + 3:TOP + Y + 3, :]
            res = rhs[p] - ys[0] * wext[0, p + 2, 3:Y + 3, :]
            for k in range(1, ROUNDS):
                x = x + ys[k] * vext[k, p + 3, TOP + 3:TOP + Y + 3, :]
                res = res - ys[k] * wext[k, p + 2, 3:Y + 3, :]
            out_x[p] = x
            out_r[p] = res

    loop(X // 4, finish)

    leave(firsts, is_sem, ir_sem)
    for r in range(ROUNDS):
        leave(back_copies(r), s_sem.at[r], r_sem.at[r])

    for k in range(n - 1):
        gram_copy(k, False).wait_send()


def on_device(gx, gy, right_side, shift):
    X, Y, Z = right_side.shape
    R = Y + 8
    n0, n1, n2 = X + 4, (X + 4) // 2, (X + 4) // 4
    n = gx * gy

    def field(*lead):
        return pltpu.VMEM(tuple(lead) + (R, Z), jnp.float32)

    def tall(*lead):
        return pltpu.VMEM(tuple(lead) + (R + 2 * TOP, Z), jnp.float32)

    def plain(*shape):
        return pltpu.VMEM(tuple(shape) + (Z,), jnp.float32)

    packed = up8(n0 * 5)
    scratch = [
        plain(X, Y), plain(X, Y),
        field(n0), field(n0), field(n0), field(n0), tall(n0 + 2), tall(n0 + 2), tall(n0 + 2),
        tall(ROUNDS, n0 + 2), tall(ROUNDS, n0 + 2), field(ROUNDS, n0),
        field(n1), field(n1), field(n1), field(n1), tall(n1 + 2), tall(n1 + 2), tall(n1 + 2),
        field(n2), field(n2), field(n2), tall(n2 + 2), tall(n2 + 2), tall(n2 + 2),
        plain(2, X // 2, 8), plain(2, 2, 2, Y), plain(2, X // 2, 8), plain(4, 8),
        plain(ROUNDS, 2, packed), field(ROUNDS, 2, 5), plain(ROUNDS, 2, packed),
        plain(ROUNDS, 4, 32), plain(n, 1),
        pltpu.SemaphoreType.DMA((2,)),
        pltpu.SemaphoreType.DMA((10,)),
        pltpu.SemaphoreType.DMA((10,)),
        pltpu.SemaphoreType.DMA((ROUNDS, 8)),
        pltpu.SemaphoreType.DMA((ROUNDS, 8)),
        pltpu.SemaphoreType.DMA((n,)),
        pltpu.SemaphoreType.DMA((n,)),
    ]
    shape = jax.ShapeDtypeStruct(right_side.shape, jnp.float32)
    return pl.pallas_call(
        functools.partial(kernel, gx, gy, X, Y, Z),
        out_shape=(shape, shape),
        in_specs=[pl.BlockSpec(memory_space=pltpu.HBM)] * 2,
        out_specs=(pl.BlockSpec(memory_space=pltpu.VMEM),) * 2,
        scratch_shapes=scratch,
        compiler_params=pltpu.CompilerParams(
            collective_id=0, has_side_effects=True, vmem_limit_bytes=VMEM_GRANT
        ),
    )(right_side, shift)


def solution(mesh):
    spec = P("gx", "gy", None)
    return jax.shard_map(
        functools.partial(on_device, mesh.shape["gx"], mesh.shape["gy"]),
        mesh=mesh, in_specs=(spec, spec), out_specs=(spec, spec), check_vma=False,
    )
```

```python
import functools

import jax
import jax.numpy as jnp
from jax import lax
from jax.experimental import pallas as pl
from jax.experimental.pallas import tpu as pltpu
from jax.sharding import PartitionSpec as P

MESH = pl.DeviceIdType.MESH
ROUNDS = 3
SWEEPS = 2
BOTTOM = 4
CENTER = 26.0
RELAX = 0.7
KEEP = 1.0 - RELAX
THETA = 1.0
TOP = 8
VMEM_GRANT = 41943040

SIDES = [(-1, 0), (1, 0), (0, -1), (0, 1)]
CORNERS = [(-1, -1), (-1, 1), (1, -1), (1, 1)]


def loop(count, body):
    def step(i, carry):
        body(i)
        return carry

    lax.fori_loop(0, count, step, 0)


def up8(k):
    return (k + 7) // 8 * 8


def kernel(
    gx, gy, X, Y, Z,
    rhs_hbm, shf_hbm, out_x, out_r,
    rhs, shf, g0, dA, wc0, cc0, e1, eA, eB, vbox, vext, wext,
    wc1, cc1, dd1, g1, e1b, eAb, eBb, wc2, cc2, g2, e1c, eAc, eBc,
    pack, in_x, in_y, in_c, ypack, rx, ry, rc, gram,
    ld_sem, is_sem, ir_sem, s_sem, r_sem, gs_sem, gr_sem,
):
    n = gx * gy
    R = Y + 8
    n0, n1, n2 = X + 4, (X + 4) // 2, (X + 4) // 4
    ix, iy = lax.axis_index("gx"), lax.axis_index("gy")
    me = ix * gy + iy
    rows = slice(TOP, TOP + R)

    def there(dx, dy):
        ok = None
        for d, i, c in ((dx, ix, gx), (dy, iy, gy)):
            if d:
                here = (i > 0) if d < 0 else (i < c - 1)
                ok = here if ok is None else jnp.logical_and(ok, here)
        return ok

    loads = [
        pltpu.make_async_copy(src, dst, ld_sem.at[k])
        for k, (src, dst) in enumerate(((rhs_hbm, rhs), (shf_hbm, shf)))
    ]
    for copy in loads:
        copy.start()
    barrier = pltpu.get_barrier_semaphore()

    xs = [ix] + [jnp.where(ix + k < gx, ix + k, ix + k - gx) for k in range(1, gx)]
    ys_at = [iy] + [jnp.where(iy + k < gy, iy + k, iy + k - gy) for k in range(1, gy)]
    others = [(a, b) for a in range(gx) for b in range(gy)][1:]
    for a, b in others:
        pl.semaphore_signal(
            barrier, inc=1, device_id=(xs[a], ys_at[b]), device_id_type=MESH
        )

    for copy in loads:
        copy.wait()

    for side, at in ((0, 0), (1, Y - 2)):
        for p in range(X // 2):
            for q in range(2):
                pack[side, p, 4 * q:4 * q + 2, :] = rhs[2 * p + q, at:at + 2, :]
                pack[side, p, 4 * q + 2:4 * q + 4, :] = shf[2 * p + q, at:at + 2, :]

    pl.semaphore_wait(barrier, n - 1)

    def remote(item, ss, rs, dx, dy):
        return pltpu.make_async_remote_copy(
            src_ref=item[2], dst_ref=item[3], send_sem=ss.at[item[4]], recv_sem=rs.at[item[5]],
            device_id=(ix + dx, iy + dy), device_id_type=MESH,
        )

    def first_copies():
        result = []
        for k, (dx, dy) in enumerate(SIDES):
            if dx:
                at = 0 if dx < 0 else X - 2
                for a, ref in enumerate((rhs, shf)):
                    result.append((dx, dy, ref.at[pl.ds(at, 2)], in_x.at[k ^ 1, a],
                                   2 * k + a, 2 * (k ^ 1) + a))
            else:
                result.append((dx, dy, pack.at[k - 2], in_y.at[(k - 2) ^ 1],
                               2 + k, 2 + (k ^ 1)))
        for k, (dx, dy) in enumerate(CORNERS):
            at = 0 if dx < 0 else X // 2 - 1
            result.append((dx, dy, pack.at[0 if dy < 0 else 1, at], in_c.at[3 - k],
                           6 + k, 6 + 3 - k))
        return result

    def depth(r):
        return 5 if r + 1 < ROUNDS else 3

    def corner_rows(r, dx):
        d = depth(r)
        if dx < 0:
            return 0, up8(d * d), 0
        base = (n0 - d) * d
        return base // 8 * 8, up8(n0 * d), base % 8

    def back_copies(r):
        result = []
        d = depth(r)
        for k, (dx, dy) in enumerate(SIDES):
            if dx:
                at = 1 if dx < 0 else X + 5 - d
                src = vbox.at[r, pl.ds(at, d), pl.ds(TOP, R)]
                result.append((dx, dy, src, rx.at[r, k ^ 1, pl.ds(0, d)], k, k ^ 1))
            else:
                tall = up8(n0 * d)
                result.append((dx, dy, ypack.at[r, k - 2, pl.ds(0, tall)],
                               ry.at[r, (k - 2) ^ 1, pl.ds(0, tall)], k, k ^ 1))
        for k, (dx, dy) in enumerate(CORNERS):
            lo, hi, _ = corner_rows(r, dx)
            src = ypack.at[r, 0 if dy < 0 else 1, pl.ds(lo, hi - lo)]
            result.append((dx, dy, src, rc.at[r, 3 - k, pl.ds(0, hi - lo)], 4 + k, 4 + 3 - k))
        return result

    def start(copies, ss, rs):
        for item in copies[::-1]:
            dx, dy = item[:2]

            @pl.when(there(dx, dy))
            def _(item=item, dx=dx, dy=dy):
                remote(item, ss, rs, dx, dy).start()

    def arrive(copies, ss, rs, use):
        for item in copies:
            dx, dy = -item[0], -item[1]

            @pl.when(there(dx, dy))
            def _(item=item, dx=dx, dy=dy):
                remote(item, ss, rs, dx, dy).wait_recv()
                use(dx, dy, item[3], item[5])

    def leave(copies, ss, rs):
        for item in copies:
            dx, dy = item[:2]

            @pl.when(there(dx, dy))
            def _(item=item, dx=dx, dy=dy):
                remote(item, ss, rs, dx, dy).wait_send()

    firsts = first_copies()
    start(firsts, is_sem, ir_sem)

    for ref in (eA, eB, e1, vbox, vext, g0, dA, eAb, eBb, e1b, eAc, eBc, e1c):
        lead = ref.shape[:-2]

        def clear(i, ref=ref, lead=lead):
            at = (i,) if len(lead) == 1 else (i // lead[1], lax.rem(i, lead[1]))
            ref[at] = jnp.zeros(ref.shape[-2:], jnp.float32)

        loop(lead[0] if len(lead) == 1 else lead[0] * lead[1], clear)

    g0[2:X + 2, 3:Y + 3, :] = rhs[...]
    dA[2:X + 2, 3:Y + 3, :] = shf[...]


    row = lax.broadcasted_iota(jnp.int32, (1, R, Z), 1)
    lane = lax.broadcasted_iota(jnp.int32, (1, R, Z), 2)
    flat_lane = lax.broadcasted_iota(jnp.int32, (R, Z), 1)

    def use_first(dx, dy, got, slot):
        s = 0 if dx < 0 else X + 2
        t = 1 if dy < 0 else Y + 3
        if dy == 0:
            (g0, dA)[slot % 2][s:s + 2, 3:Y + 3, :] = got[...]
            return
        for a, ref in enumerate((g0, dA)):
            if dx == 0:
                for i in range(X):
                    q = 4 * (i % 2) + 2 * a
                    ref[2 + i, t:t + 2, :] = got[i // 2, q:q + 2, :]
            else:
                for q in range(2):
                    p = 4 * q + 2 * a
                    ref[s + q, t:t + 2, :] = got[p:p + 2, :]

    arrive(firsts, is_sem, ir_sem, use_first)

    in_box = jnp.logical_and(row >= 1, row <= Y + 4)
    relax = jnp.where(in_box, RELAX, 0.0).astype(jnp.float32)
    at_y = iy * Y + row - 3
    in_grid = jnp.where(
        jnp.logical_and(at_y >= 0, at_y < gy * Y), 1.0, 0.0
    ).astype(jnp.float32)

    def pair_sum(t, k):
        first = lax.rem(jnp.maximum(row - 1, 0) // k, 2) == 0
        t = t + jnp.where(first, pltpu.roll(t, R - k, 1), pltpu.roll(t, k, 1))
        low = lax.rem(lane // k, 2) == 0
        return t + jnp.where(low, pltpu.roll(t, Z - k, 2), pltpu.roll(t, k, 2))

    def cube(src, at, ch, k):
        last = []
        for j in range(ch + 2):
            got = src[at + j, rows, :]
            t = got + (src[at + j, TOP - k:TOP - k + R, :] + src[at + j, TOP + k:TOP + k + R, :])
            last.append((got, t))
            if j >= 2:
                t = last[0][1] + last[1][1] + last[2][1]
                up = jnp.where(flat_lane >= k, pltpu.roll(t, k, 1), 0.0)
                down = jnp.where(flat_lane < Z - k, pltpu.roll(t, Z - k, 1), 0.0)
                yield j - 2, last[1][0], t + (up + down)
                last = last[1:]

    def mean_shift(i):
        for j in range(5):
            s = dA[pl.ds(10 * i + 2 * j, 2)]
            dd1[pl.ds(5 * i + j, 1)] = pair_sum(s[0:1] + s[1:2], 1) * 0.125

    loop(n1 // 5, mean_shift)

    def weights(wc, cc, dp, count, values):
        def body(i):
            for j in range(5):
                at = pl.ds(5 * i + j, 1)
                d = CENTER + values(5 * i + j)
                w = relax / d
                wc[at] = w
                cc[at] = KEEP - w
                if dp is not None:
                    dp[at] = d + 1.0

        loop(count // 5, body)

    def mean_second(i):
        s = dd1[pl.ds(2 * i, 2)]
        return 16.0 * (pair_sum(s[0:1] + s[1:2], 2) * 0.125)

    weights(wc0, cc0, dA, n0, lambda i: dA[pl.ds(i, 1)])
    weights(wc2, cc2, None, n2, mean_second)
    weights(wc1, cc1, dd1, n1, lambda i: 4.0 * dd1[pl.ds(i, 1)])

    def scaled(dst, src, wc, count, ch):
        def body(i):
            at = i * ch
            dst[pl.ds(at + 1, ch), rows, :] = wc[pl.ds(at, ch)] * src[pl.ds(at, ch)]

        loop(count // ch, body)

    def sweep(dst, src, wg, wc, cc, count, k, ch):
        def body(i):
            at = i * ch
            for j, mid, s in cube(src, at, ch, k):
                base = mid if wg is src else wg[at + j + 1, rows, :]
                dst[at + j + 1, rows, :] = cc[at + j] * mid + base + wc[at + j] * s

        loop(count // ch, body)

    def down(dst, src, g, dp, count, k, ch):
        def body(i):
            at = i * ch
            for j, mid, s in cube(src, at, ch, k):
                left = g[at + j] - dp[at + j] * mid + s
                if j % 2:
                    dst[i * (ch // 2) + j // 2] = 0.5 * pair_sum((held + left)[None], k)[0]
                held = left

        loop(count // ch, body)

    def up(dst, src, count):
        def body(i):
            dst[pl.ds(2 * i + 1, 2), rows, :] = (
                dst[pl.ds(2 * i + 1, 2), rows, :] + src[pl.ds(i + 1, 1), rows, :]
            )

        loop(count // 2, body)

    h0 = n0 // 2

    def vcycle(dst, g):
        sweep(eA, e1, e1, wc0, cc0, n0, 1, h0)
        down(g1, eA, g, dA, n0, 1, h0)
        scaled(e1b, g1, wc1, n1, n1)
        sweep(eAb, e1b, e1b, wc1, cc1, n1, 2, n1)
        down(g2, eAb, g1, dd1, n1, 2, n1)
        scaled(e1c, g2, wc2, n2, n2)
        sweep(eAc, e1c, e1c, wc2, cc2, n2, 4, n2)
        for turn in range(BOTTOM - 2):
            a, b = (eBc, eAc) if turn % 2 == 0 else (eAc, eBc)
            sweep(a, b, e1c, wc2, cc2, n2, 4, n2)
        up(eAb, eAc, n1)
        sweep(eBb, eAb, e1b, wc1, cc1, n1, 2, n1)
        sweep(eAb, eBb, e1b, wc1, cc1, n1, 2, n1)
        up(eA, eAb, n0)
        sweep(eB, eA, e1, wc0, cc0, n0, 1, h0)
        sweep(dst, eB, e1, wc0, cc0, n0, 1, h0)

    own = jnp.where(jnp.logical_and(row >= 3, row < Y + 3), 1.0, 0.0).astype(jnp.float32)

    def dots(r):
        ch = 4

        def body(i, sums):
            w = own * wext[r, pl.ds(ch * i + 2, ch)]
            terms = [own * g0[pl.ds(ch * i + 2, ch)] * vext[r, pl.ds(ch * i + 3, ch), rows, :]]
            terms += [vext[a, pl.ds(ch * i + 3, ch), rows, :] * w for a in range(r + 1)]
            return tuple(
                s + jnp.sum(t.reshape(ch * R // 8, 8, Z), axis=0) for s, t in zip(sums, terms)
            )

        zero = jnp.zeros((8, Z), jnp.float32)
        return lax.fori_loop(0, X // ch, body, (zero,) * (r + 2))

    scaled(e1, g0, wc0, n0, 4)
    sums = []
    for r in range(ROUNDS):
        vcycle(vbox.at[r], g0 if r == 0 else wext.at[r - 1])
        d = depth(r)
        for i in range(n0):
            ypack[r, 0, d * i:d * i + d, :] = vbox[r, i + 1, TOP + 1:TOP + 1 + d, :]
            ypack[r, 1, d * i:d * i + d, :] = vbox[r, i + 1, TOP + Y + 5 - d:TOP + Y + 5, :]
        copies = back_copies(r)
        ss, rs = s_sem.at[r], r_sem.at[r]
        start(copies, ss, rs)

        v = vext.at[r]

        def take(i):
            at = pl.ds(2 * i, 2)
            t = vbox[r, at, rows, :] * in_grid
            if r:
                t = t - THETA * vext[r - 1, at, rows, :]
            v[at, rows, :] = t

        loop((n0 + 2) // 2, take)
        if r:
            sums.append(dots(r - 1))

        def use_back(dx, dy, got, slot):
            s = 5 - d if dx < 0 else X + 1
            t = TOP + 5 - d if dy < 0 else TOP + Y + 1
            if dy == 0:
                v[s:s + d, rows, :] = v[s:s + d, rows, :] + got[...] * in_grid
                return
            skip = 0 if dx == 0 else corner_rows(r, -dx)[2]
            if dx == 0:
                s = 1
            for j in range(n0 if dx == 0 else d):
                v[s + j, t:t + d, :] = (
                    v[s + j, t:t + d, :] + got[skip + d * j:skip + d * j + d, :]
                )

        arrive(copies, ss, rs, use_back)

        @pl.when(ix == 0)
        def _():
            v[0:3, rows, :] = jnp.zeros((3, R, Z), jnp.float32)

        @pl.when(ix == gx - 1)
        def _():
            v[X + 3:X + 6, rows, :] = jnp.zeros((3, R, Z), jnp.float32)

        w = wext.at[r]
        last = r + 1 == ROUNDS

        def apply(i):
            ch = X // 2 if last else h0
            at = i * ch + (2 if last else 0)
            for j, mid, s in cube(v, at, ch, 1):
                t = in_grid[0] * (dA[at + j] * mid - s)
                w[at + j] = t
                if not last:
                    e1[at + j + 1, rows, :] = wc0[at + j] * t

        loop(2, apply)

        if not last:
            for edge, at in ((0, 0), (gx - 1, X + 2)):
                @pl.when(ix == edge)
                def _(at=at):
                    w[at:at + 2] = jnp.zeros((2, R, Z), jnp.float32)
                    e1[at + 1:at + 3, rows, :] = jnp.zeros((2, R, Z), jnp.float32)

    sums.append(dots(ROUNDS - 1))
    flat = [t for group in sums for t in group]
    line = lax.broadcasted_iota(jnp.int32, (1, Z), 1)
    packed = jnp.zeros((1, Z), jnp.float32)
    for k, s in enumerate(flat):
        total = jnp.sum(jnp.sum(s, axis=0, keepdims=True), axis=1, keepdims=True)
        packed = jnp.where(line == k, total, packed)
    gram[me] = packed

    def gram_copy(k, back):
        a, b = others[k]
        slot = me
        if back:
            slot = xs[(gx - a) % gx] * gy + ys_at[(gy - b) % gy]
        return pltpu.make_async_remote_copy(
            src_ref=gram.at[me], dst_ref=gram.at[slot],
            send_sem=gs_sem.at[k], recv_sem=gr_sem.at[slot],
            device_id=(xs[a], ys_at[b]), device_id_type=MESH,
        )

    for k in range(n - 1)[::-1]:
        gram_copy(k, False).start()
    for k in range(n - 1):
        gram_copy(k, True).wait_recv()

    total = jnp.sum(gram[...], axis=0)
    b0, g00, b1, g01, g11, b2, g02, g12, g22 = [
        jnp.broadcast_to(
            jnp.sum(jnp.where(line == k, total, 0.0), axis=1, keepdims=True), (1, Z)
        )
        for k in range(9)
    ]
    l1, l2 = g01 / g00, g02 / g00
    d1 = g11 - l1 * g01
    f12 = g12 - l1 * g02
    l3 = f12 / d1
    d2 = g22 - l2 * g02 - l3 * f12
    c1 = b1 - l1 * b0
    c2 = b2 - l2 * b0 - l3 * c1
    y2 = c2 / d2
    y1 = (c1 - f12 * y2) / d1
    y0 = (b0 - g01 * y1 - g02 * y2) / g00
    ys = [jnp.broadcast_to(t, (Y, Z)) for t in (y0, y1, y2)]

    def finish(i):
        for j in range(4):
            p = 4 * i + j
            x = ys[0] * vext[0, p + 3, TOP + 3:TOP + Y + 3, :]
            res = rhs[p] - ys[0] * wext[0, p + 2, 3:Y + 3, :]
            for k in range(1, ROUNDS):
                x = x + ys[k] * vext[k, p + 3, TOP + 3:TOP + Y + 3, :]
                res = res - ys[k] * wext[k, p + 2, 3:Y + 3, :]
            out_x[p] = x
            out_r[p] = res

    loop(X // 4, finish)

    leave(firsts, is_sem, ir_sem)
    for r in range(ROUNDS):
        leave(back_copies(r), s_sem.at[r], r_sem.at[r])

    for k in range(n - 1):
        gram_copy(k, False).wait_send()


def on_device(gx, gy, right_side, shift):
    X, Y, Z = right_side.shape
    R = Y + 8
    n0, n1, n2 = X + 4, (X + 4) // 2, (X + 4) // 4
    n = gx * gy

    def field(*lead):
        return pltpu.VMEM(tuple(lead) + (R, Z), jnp.float32)

    def tall(*lead):
        return pltpu.VMEM(tuple(lead) + (R + 2 * TOP, Z), jnp.float32)

    def plain(*shape):
        return pltpu.VMEM(tuple(shape) + (Z,), jnp.float32)

    packed = up8(n0 * 5)
    scratch = [
        plain(X, Y), plain(X, Y),
        field(n0), field(n0), field(n0), field(n0), tall(n0 + 2), tall(n0 + 2), tall(n0 + 2),
        tall(ROUNDS, n0 + 2), tall(ROUNDS, n0 + 2), field(ROUNDS, n0),
        field(n1), field(n1), field(n1), field(n1), tall(n1 + 2), tall(n1 + 2), tall(n1 + 2),
        field(n2), field(n2), field(n2), tall(n2 + 2), tall(n2 + 2), tall(n2 + 2),
        plain(2, X // 2, 8), plain(2, 2, 2, Y), plain(2, X // 2, 8), plain(4, 8),
        plain(ROUNDS, 2, packed), field(ROUNDS, 2, 5), plain(ROUNDS, 2, packed),
        plain(ROUNDS, 4, 32), plain(n, 1),
        pltpu.SemaphoreType.DMA((2,)),
        pltpu.SemaphoreType.DMA((10,)),
        pltpu.SemaphoreType.DMA((10,)),
        pltpu.SemaphoreType.DMA((ROUNDS, 8)),
        pltpu.SemaphoreType.DMA((ROUNDS, 8)),
        pltpu.SemaphoreType.DMA((n,)),
        pltpu.SemaphoreType.DMA((n,)),
    ]
    shape = jax.ShapeDtypeStruct(right_side.shape, jnp.float32)
    return pl.pallas_call(
        functools.partial(kernel, gx, gy, X, Y, Z),
        out_shape=(shape, shape),
        in_specs=[pl.BlockSpec(memory_space=pltpu.HBM)] * 2,
        out_specs=(pl.BlockSpec(memory_space=pltpu.VMEM),) * 2,
        scratch_shapes=scratch,
        compiler_params=pltpu.CompilerParams(
            collective_id=0, has_side_effects=True, vmem_limit_bytes=VMEM_GRANT
        ),
    )(*(pltpu.with_memory_space_constraint(t, pltpu.HBM) for t in (right_side, shift)))


def solution(mesh):
    spec = P("gx", "gy", None)
    return jax.shard_map(
        functools.partial(on_device, mesh.shape["gx"], mesh.shape["gy"]),
        mesh=mesh, in_specs=(spec, spec), out_specs=(spec, spec), check_vma=False,
    )
```

```python
import functools

import jax
import jax.numpy as jnp
from jax import lax
from jax.experimental import pallas as pl
from jax.experimental.pallas import tpu as pltpu
from jax.sharding import PartitionSpec as P

MESH = pl.DeviceIdType.MESH
ROUNDS = 3
SWEEPS = 2
BOTTOM = 4
CENTER = 26.0
RELAX = 0.7
KEEP = 1.0 - RELAX
THETA = 1.0
TOP = 8
VMEM_GRANT = 41943040

SIDES = [(-1, 0), (1, 0), (0, -1), (0, 1)]
CORNERS = [(-1, -1), (-1, 1), (1, -1), (1, 1)]


def loop(count, body):
    def step(i, carry):
        body(i)
        return carry

    lax.fori_loop(0, count, step, 0)


def up8(k):
    return (k + 7) // 8 * 8


def kernel(
    gx, gy, X, Y, Z,
    rhs_hbm, shf_hbm, out_x, out_r,
    rhs, shf, dA, wc0, cc0, e1, eA, eB, vbox, vext, wext,
    wc1, cc1, dd1, g1, e1b, eAb, eBb, wc2, cc2, g2, e1c, eAc, eBc,
    partial, pack, in_x, in_y, in_c, ypack, rx, ry, rc, gram,
    ld_sem, is_sem, ir_sem, s_sem, r_sem, gs_sem, gr_sem,
):
    n = gx * gy
    R = Y + 8
    n0, n1, n2 = X + 4, (X + 4) // 2, (X + 4) // 4
    ix, iy = lax.axis_index("gx"), lax.axis_index("gy")
    me = ix * gy + iy
    rows = slice(TOP, TOP + R)
    g0 = wext.at[0]

    def there(dx, dy):
        ok = None
        for d, i, c in ((dx, ix, gx), (dy, iy, gy)):
            if d:
                here = (i > 0) if d < 0 else (i < c - 1)
                ok = here if ok is None else jnp.logical_and(ok, here)
        return ok

    loads = [
        pltpu.make_async_copy(src, dst, ld_sem.at[k])
        for k, (src, dst) in enumerate(((rhs_hbm, rhs), (shf_hbm, shf)))
    ]
    for copy in loads:
        copy.start()
    barrier = pltpu.get_barrier_semaphore()

    xs = [ix] + [jnp.where(ix + k < gx, ix + k, ix + k - gx) for k in range(1, gx)]
    ys_at = [iy] + [jnp.where(iy + k < gy, iy + k, iy + k - gy) for k in range(1, gy)]
    others = [(a, b) for a in range(gx) for b in range(gy)][1:]
    for a, b in others:
        pl.semaphore_signal(
            barrier, inc=1, device_id=(xs[a], ys_at[b]), device_id_type=MESH
        )

    for copy in loads:
        copy.wait()

    for side, at in ((0, 0), (1, Y - 2)):
        for p in range(X // 2):
            for q in range(2):
                pack[side, p, 4 * q:4 * q + 2, :] = rhs[2 * p + q, at:at + 2, :]
                pack[side, p, 4 * q + 2:4 * q + 4, :] = shf[2 * p + q, at:at + 2, :]

    pl.semaphore_wait(barrier, n - 1)

    def remote(item, ss, rs, dx, dy):
        return pltpu.make_async_remote_copy(
            src_ref=item[2], dst_ref=item[3], send_sem=ss.at[item[4]], recv_sem=rs.at[item[5]],
            device_id=(ix + dx, iy + dy), device_id_type=MESH,
        )

    def first_copies():
        result = []
        for k, (dx, dy) in enumerate(SIDES):
            if dx:
                at = 0 if dx < 0 else X - 2
                for a, ref in enumerate((rhs, shf)):
                    result.append((dx, dy, ref.at[pl.ds(at, 2)], in_x.at[k ^ 1, a],
                                   2 * k + a, 2 * (k ^ 1) + a))
            else:
                result.append((dx, dy, pack.at[k - 2], in_y.at[(k - 2) ^ 1],
                               2 + k, 2 + (k ^ 1)))
        for k, (dx, dy) in enumerate(CORNERS):
            at = 0 if dx < 0 else X // 2 - 1
            result.append((dx, dy, pack.at[0 if dy < 0 else 1, at], in_c.at[3 - k],
                           6 + k, 6 + 3 - k))
        return result

    def depth(r):
        return 5 if r + 1 < ROUNDS else 3

    def corner_rows(r, dx):
        d = depth(r)
        if dx < 0:
            return 0, up8(d * d), 0
        base = (n0 - d) * d
        return base // 8 * 8, up8(n0 * d), base % 8

    def back_copies(r):
        result = []
        d = depth(r)
        for k, (dx, dy) in enumerate(SIDES):
            if dx:
                at = 1 if dx < 0 else X + 5 - d
                src = vbox.at[r, pl.ds(at, d), pl.ds(TOP, R)]
                result.append((dx, dy, src, rx.at[r, k ^ 1, pl.ds(0, d)], k, k ^ 1))
            else:
                tall = up8(n0 * d)
                result.append((dx, dy, ypack.at[r, k - 2, pl.ds(0, tall)],
                               ry.at[r, (k - 2) ^ 1, pl.ds(0, tall)], k, k ^ 1))
        for k, (dx, dy) in enumerate(CORNERS):
            lo, hi, _ = corner_rows(r, dx)
            src = ypack.at[r, 0 if dy < 0 else 1, pl.ds(lo, hi - lo)]
            result.append((dx, dy, src, rc.at[r, 3 - k, pl.ds(0, hi - lo)], 4 + k, 4 + 3 - k))
        return result

    def start(copies, ss, rs):
        for item in copies[::-1]:
            dx, dy = item[:2]

            @pl.when(there(dx, dy))
            def _(item=item, dx=dx, dy=dy):
                remote(item, ss, rs, dx, dy).start()

    def arrive(copies, ss, rs, use):
        for item in copies:
            dx, dy = -item[0], -item[1]

            @pl.when(there(dx, dy))
            def _(item=item, dx=dx, dy=dy):
                remote(item, ss, rs, dx, dy).wait_recv()
                use(dx, dy, item[3], item[5])

    def leave(copies, ss, rs):
        for item in copies:
            dx, dy = item[:2]

            @pl.when(there(dx, dy))
            def _(item=item, dx=dx, dy=dy):
                remote(item, ss, rs, dx, dy).wait_send()

    firsts = first_copies()
    start(firsts, is_sem, ir_sem)

    for ref in (eA, eB, e1, vbox, vext, g0, dA, eAb, eBb, e1b, eAc, eBc, e1c):
        lead = ref.shape[:-2]

        def clear(i, ref=ref, lead=lead):
            at = (i,) if len(lead) == 1 else (i // lead[1], lax.rem(i, lead[1]))
            ref[at] = jnp.zeros(ref.shape[-2:], jnp.float32)

        loop(lead[0] if len(lead) == 1 else lead[0] * lead[1], clear)

    g0[2:X + 2, 3:Y + 3, :] = rhs[...]
    dA[2:X + 2, 3:Y + 3, :] = shf[...]


    row = lax.broadcasted_iota(jnp.int32, (1, R, Z), 1)
    lane = lax.broadcasted_iota(jnp.int32, (1, R, Z), 2)
    flat_lane = lax.broadcasted_iota(jnp.int32, (R, Z), 1)

    def use_first(dx, dy, got, slot):
        s = 0 if dx < 0 else X + 2
        t = 1 if dy < 0 else Y + 3
        if dy == 0:
            (g0, dA)[slot % 2][s:s + 2, 3:Y + 3, :] = got[...]
            return
        for a, ref in enumerate((g0, dA)):
            if dx == 0:
                for i in range(X):
                    q = 4 * (i % 2) + 2 * a
                    ref[2 + i, t:t + 2, :] = got[i // 2, q:q + 2, :]
            else:
                for q in range(2):
                    p = 4 * q + 2 * a
                    ref[s + q, t:t + 2, :] = got[p:p + 2, :]

    arrive(firsts, is_sem, ir_sem, use_first)

    in_box = jnp.logical_and(row >= 1, row <= Y + 4)
    relax = jnp.where(in_box, RELAX, 0.0).astype(jnp.float32)
    at_y = iy * Y + row - 3
    in_grid = jnp.where(
        jnp.logical_and(at_y >= 0, at_y < gy * Y), 1.0, 0.0
    ).astype(jnp.float32)

    def pair_sum(t, k):
        first = lax.rem(jnp.maximum(row - 1, 0) // k, 2) == 0
        t = t + jnp.where(first, pltpu.roll(t, R - k, 1), pltpu.roll(t, k, 1))
        low = lax.rem(lane // k, 2) == 0
        return t + jnp.where(low, pltpu.roll(t, Z - k, 2), pltpu.roll(t, k, 2))

    def cube(src, at, ch, k):
        last = []
        for j in range(ch + 2):
            got = src[at + j, rows, :]
            t = got + (src[at + j, TOP - k:TOP - k + R, :] + src[at + j, TOP + k:TOP + k + R, :])
            last.append((got, t))
            if j >= 2:
                t = last[0][1] + last[1][1] + last[2][1]
                up = jnp.where(flat_lane >= k, pltpu.roll(t, k, 1), 0.0)
                down = jnp.where(flat_lane < Z - k, pltpu.roll(t, Z - k, 1), 0.0)
                yield j - 2, last[1][0], t + (up + down)
                last = last[1:]

    def mean_shift(i):
        for j in range(5):
            s = dA[pl.ds(10 * i + 2 * j, 2)]
            dd1[pl.ds(5 * i + j, 1)] = pair_sum(s[0:1] + s[1:2], 1) * 0.125

    loop(n1 // 5, mean_shift)

    def weights(wc, cc, dp, count, values):
        def body(i):
            for j in range(5):
                at = pl.ds(5 * i + j, 1)
                d = CENTER + values(5 * i + j)
                w = relax / d
                wc[at] = w
                cc[at] = KEEP - w
                if dp is not None:
                    dp[at] = d + 1.0

        loop(count // 5, body)

    def mean_second(i):
        s = dd1[pl.ds(2 * i, 2)]
        return 16.0 * (pair_sum(s[0:1] + s[1:2], 2) * 0.125)

    weights(wc0, cc0, dA, n0, lambda i: dA[pl.ds(i, 1)])
    weights(wc2, cc2, None, n2, mean_second)
    weights(wc1, cc1, dd1, n1, lambda i: 4.0 * dd1[pl.ds(i, 1)])

    def scaled(dst, src, wc, count, ch):
        def body(i):
            at = i * ch
            dst[pl.ds(at + 1, ch), rows, :] = wc[pl.ds(at, ch)] * src[pl.ds(at, ch)]

        loop(count // ch, body)

    def sweep(dst, src, wg, wc, cc, count, k, ch):
        def body(i):
            at = i * ch
            for j, mid, s in cube(src, at, ch, k):
                base = mid if wg is src else wg[at + j + 1, rows, :]
                dst[at + j + 1, rows, :] = cc[at + j] * mid + base + wc[at + j] * s

        loop(count // ch, body)

    def down(dst, src, g, dp, count, k, ch):
        def body(i):
            at = i * ch
            for j, mid, s in cube(src, at, ch, k):
                left = g[at + j] - dp[at + j] * mid + s
                if j % 2:
                    dst[i * (ch // 2) + j // 2] = 0.5 * pair_sum((held + left)[None], k)[0]
                held = left

        loop(count // ch, body)

    def up(dst, src, count):
        def body(i):
            dst[pl.ds(2 * i + 1, 2), rows, :] = (
                dst[pl.ds(2 * i + 1, 2), rows, :] + src[pl.ds(i + 1, 1), rows, :]
            )

        loop(count // 2, body)

    h0 = n0 // 2

    def vcycle(dst, g):
        sweep(eA, e1, e1, wc0, cc0, n0, 1, h0)
        down(g1, eA, g, dA, n0, 1, h0)
        scaled(e1b, g1, wc1, n1, n1)
        sweep(eAb, e1b, e1b, wc1, cc1, n1, 2, n1)
        down(g2, eAb, g1, dd1, n1, 2, n1)
        scaled(e1c, g2, wc2, n2, n2)
        sweep(eAc, e1c, e1c, wc2, cc2, n2, 4, n2)
        for turn in range(BOTTOM - 2):
            a, b = (eBc, eAc) if turn % 2 == 0 else (eAc, eBc)
            sweep(a, b, e1c, wc2, cc2, n2, 4, n2)
        up(eAb, eAc, n1)
        sweep(eBb, eAb, e1b, wc1, cc1, n1, 2, n1)
        sweep(eAb, eBb, e1b, wc1, cc1, n1, 2, n1)
        up(eA, eAb, n0)
        sweep(eB, eA, e1, wc0, cc0, n0, 1, h0)
        sweep(dst, eB, e1, wc0, cc0, n0, 1, h0)

    own = jnp.where(jnp.logical_and(row >= 3, row < Y + 3), 1.0, 0.0).astype(jnp.float32)

    def dots(r):
        ch = 4

        def body(i, sums):
            w = own * wext[r + 1, pl.ds(ch * i + 2, ch)]
            terms = [own * g0[pl.ds(ch * i + 2, ch)] * vext[r, pl.ds(ch * i + 3, ch), rows, :]]
            terms += [vext[a, pl.ds(ch * i + 3, ch), rows, :] * w for a in range(r + 1)]
            return tuple(
                s + jnp.sum(t.reshape(ch * R // 8, 8, Z), axis=0) for s, t in zip(sums, terms)
            )

        zero = jnp.zeros((8, Z), jnp.float32)
        done = lax.fori_loop(0, X // ch, body, (zero,) * (r + 2))
        for k, t in enumerate(done):
            partial[r * (r + 3) // 2 + k] = t

    scaled(e1, g0, wc0, n0, 4)
    def exchange(r):
        d = depth(r)
        for i in range(n0):
            ypack[r, 0, d * i:d * i + d, :] = vbox[r, i + 1, TOP + 1:TOP + 1 + d, :]
            ypack[r, 1, d * i:d * i + d, :] = vbox[r, i + 1, TOP + Y + 5 - d:TOP + Y + 5, :]
        copies = back_copies(r)
        ss, rs = s_sem.at[r], r_sem.at[r]
        start(copies, ss, rs)

        v = vext.at[r]

        def take(i):
            at = pl.ds(2 * i, 2)
            t = vbox[r, at, rows, :] * in_grid
            if r:
                t = t - THETA * vext[r - 1, at, rows, :]
            v[at, rows, :] = t

        loop((n0 + 2) // 2, take)
        if r:
            dots(r - 1)

        def use_back(dx, dy, got, slot):
            s = 5 - d if dx < 0 else X + 1
            t = TOP + 5 - d if dy < 0 else TOP + Y + 1
            if dy == 0:
                v[s:s + d, rows, :] = v[s:s + d, rows, :] + got[...] * in_grid
                return
            skip = 0 if dx == 0 else corner_rows(r, -dx)[2]
            if dx == 0:
                s = 1
            for j in range(n0 if dx == 0 else d):
                v[s + j, t:t + d, :] = (
                    v[s + j, t:t + d, :] + got[skip + d * j:skip + d * j + d, :]
                )

        arrive(copies, ss, rs, use_back)

        @pl.when(ix == 0)
        def _():
            v[0:3, rows, :] = jnp.zeros((3, R, Z), jnp.float32)

        @pl.when(ix == gx - 1)
        def _():
            v[X + 3:X + 6, rows, :] = jnp.zeros((3, R, Z), jnp.float32)

        w = wext.at[r + 1]
        last = r + 1 == ROUNDS

        def apply(i):
            ch = X // 2 if last else h0
            at = i * ch + (2 if last else 0)
            for j, mid, s in cube(v, at, ch, 1):
                t = in_grid[0] * (dA[at + j] * mid - s)
                w[at + j] = t
                if not last:
                    e1[at + j + 1, rows, :] = wc0[at + j] * t

        loop(2, apply)

        if not last:
            for edge, at in ((0, 0), (gx - 1, X + 2)):
                @pl.when(ix == edge)
                def _(at=at):
                    w[at:at + 2] = jnp.zeros((2, R, Z), jnp.float32)
                    e1[at + 1:at + 3, rows, :] = jnp.zeros((2, R, Z), jnp.float32)

    def one_round(now):
        vcycle(vbox.at[now], wext.at[now])
        for r in range(ROUNDS):
            @pl.when(now == r)
            def _(r=r):
                exchange(r)

    loop(ROUNDS, one_round)
    dots(ROUNDS - 1)
    line = lax.broadcasted_iota(jnp.int32, (1, Z), 1)
    packed = jnp.zeros((1, Z), jnp.float32)
    for k in range(9):
        total = jnp.sum(jnp.sum(partial[k], axis=0, keepdims=True), axis=1, keepdims=True)
        packed = jnp.where(line == k, total, packed)
    gram[me] = packed

    def gram_copy(k, back):
        a, b = others[k]
        slot = me
        if back:
            slot = xs[(gx - a) % gx] * gy + ys_at[(gy - b) % gy]
        return pltpu.make_async_remote_copy(
            src_ref=gram.at[me], dst_ref=gram.at[slot],
            send_sem=gs_sem.at[k], recv_sem=gr_sem.at[slot],
            device_id=(xs[a], ys_at[b]), device_id_type=MESH,
        )

    for k in range(n - 1)[::-1]:
        gram_copy(k, False).start()
    for k in range(n - 1):
        gram_copy(k, True).wait_recv()

    total = jnp.sum(gram[...], axis=0)
    b0, g00, b1, g01, g11, b2, g02, g12, g22 = [
        jnp.broadcast_to(
            jnp.sum(jnp.where(line == k, total, 0.0), axis=1, keepdims=True), (1, Z)
        )
        for k in range(9)
    ]
    l1, l2 = g01 / g00, g02 / g00
    d1 = g11 - l1 * g01
    f12 = g12 - l1 * g02
    l3 = f12 / d1
    d2 = g22 - l2 * g02 - l3 * f12
    c1 = b1 - l1 * b0
    c2 = b2 - l2 * b0 - l3 * c1
    y2 = c2 / d2
    y1 = (c1 - f12 * y2) / d1
    y0 = (b0 - g01 * y1 - g02 * y2) / g00
    ys = [jnp.broadcast_to(t, (Y, Z)) for t in (y0, y1, y2)]

    def finish(i):
        for j in range(4):
            p = 4 * i + j
            x = ys[0] * vext[0, p + 3, TOP + 3:TOP + Y + 3, :]
            res = rhs[p] - ys[0] * wext[1, p + 2, 3:Y + 3, :]
            for k in range(1, ROUNDS):
                x = x + ys[k] * vext[k, p + 3, TOP + 3:TOP + Y + 3, :]
                res = res - ys[k] * wext[k + 1, p + 2, 3:Y + 3, :]
            out_x[p] = x
            out_r[p] = res

    loop(X // 4, finish)

    leave(firsts, is_sem, ir_sem)
    for r in range(ROUNDS):
        leave(back_copies(r), s_sem.at[r], r_sem.at[r])

    for k in range(n - 1):
        gram_copy(k, False).wait_send()


def on_device(gx, gy, right_side, shift):
    X, Y, Z = right_side.shape
    R = Y + 8
    n0, n1, n2 = X + 4, (X + 4) // 2, (X + 4) // 4
    n = gx * gy

    def field(*lead):
        return pltpu.VMEM(tuple(lead) + (R, Z), jnp.float32)

    def tall(*lead):
        return pltpu.VMEM(tuple(lead) + (R + 2 * TOP, Z), jnp.float32)

    def plain(*shape):
        return pltpu.VMEM(tuple(shape) + (Z,), jnp.float32)

    packed = up8(n0 * 5)
    scratch = [
        plain(X, Y), plain(X, Y),
        field(n0), field(n0), field(n0), tall(n0 + 2), tall(n0 + 2), tall(n0 + 2),
        tall(ROUNDS, n0 + 2), tall(ROUNDS, n0 + 2), field(ROUNDS + 1, n0),
        field(n1), field(n1), field(n1), field(n1), tall(n1 + 2), tall(n1 + 2), tall(n1 + 2),
        field(n2), field(n2), field(n2), tall(n2 + 2), tall(n2 + 2), tall(n2 + 2),
        plain(9, 8), plain(2, X // 2, 8), plain(2, 2, 2, Y), plain(2, X // 2, 8), plain(4, 8),
        plain(ROUNDS, 2, packed), field(ROUNDS, 2, 5), plain(ROUNDS, 2, packed),
        plain(ROUNDS, 4, 32), plain(n, 1),
        pltpu.SemaphoreType.DMA((2,)),
        pltpu.SemaphoreType.DMA((10,)),
        pltpu.SemaphoreType.DMA((10,)),
        pltpu.SemaphoreType.DMA((ROUNDS, 8)),
        pltpu.SemaphoreType.DMA((ROUNDS, 8)),
        pltpu.SemaphoreType.DMA((n,)),
        pltpu.SemaphoreType.DMA((n,)),
    ]
    shape = jax.ShapeDtypeStruct(right_side.shape, jnp.float32)
    return pl.pallas_call(
        functools.partial(kernel, gx, gy, X, Y, Z),
        out_shape=(shape, shape),
        in_specs=[pl.BlockSpec(memory_space=pltpu.HBM)] * 2,
        out_specs=(pl.BlockSpec(memory_space=pltpu.VMEM),) * 2,
        scratch_shapes=scratch,
        compiler_params=pltpu.CompilerParams(
            collective_id=0, has_side_effects=True, vmem_limit_bytes=VMEM_GRANT
        ),
    )(*(pltpu.with_memory_space_constraint(t, pltpu.HBM) for t in (right_side, shift)))


def solution(mesh):
    spec = P("gx", "gy", None)
    return jax.shard_map(
        functools.partial(on_device, mesh.shape["gx"], mesh.shape["gy"]),
        mesh=mesh, in_specs=(spec, spec), out_specs=(spec, spec), check_vma=False,
    )
```
